32 devices in a mesh: data: 1 (over z), ffn: 4 (over y), hid: 8 (over x, core).
Axes of the slice: x: 4, y: 4, z: 1, core: 2. Of those that a mesh axis runs over, the one named last changes fastest.
The devices are a block of a 4x4x8 slice.
Arguments:
- residual: bfloat16 [4096, 4096], P('data', 'hid')
- gain_mlp: float32 [4096], P('hid')
- gain_attn: float32 [4096], P('hid')
- w_gate: bfloat16 [4096, 14336], P('hid', 'ffn')
- w_up: bfloat16 [4096, 14336], P('hid', 'ffn')
- w_down: bfloat16 [14336, 4096], P('ffn', 'hid')
- w_qkv: bfloat16 [4096, 6144], P('hid', 'ffn')
Outputs:
- output 1: bfloat16 [4096, 4096], P('data', 'hid')
- output 2: bfloat16 [4096, 6144], P('data', 'ffn')
All inputs are finite; a program needn't handle non-finite values.
Results may differ from the reference program's by a relative error of at most 0.02.
Values are sent between devices in bfloat16 or wider.
A program may use at most 768 MiB of HBM per device.

```python
import jax
import jax.numpy as jnp
from jax import lax

TOKENS = 4096
D_MODEL = 4096
D_FF = 14336
Q_HEADS = 32
KV_HEADS = 8
HEAD_DIM = 128
HID_WAYS = 8
FFN_WAYS = 4
QKV_DIM = (Q_HEADS + 2 * KV_HEADS) * HEAD_DIM
NORM_EPS = 1e-6


def setup_inputs(seed: int = 0, part: int = 0) -> dict:
    keys = jax.random.split(jax.random.key(seed), 8)
    part_keys = jax.random.split(jax.random.fold_in(keys[0], part), 4)
    d_shard = D_MODEL // HID_WAYS
    noise = jax.random.normal(part_keys[0], (TOKENS, HID_WAYS, d_shard), jnp.float32)
    row_scale = jnp.exp(jax.random.uniform(part_keys[1], (TOKENS, 1, 1), jnp.float32, minval=-1.0, maxval=1.0))
    block_scale = jnp.exp(jax.random.uniform(part_keys[2], (TOKENS, HID_WAYS, 1), jnp.float32, minval=-0.7, maxval=0.7))
    col_scale = jnp.exp(0.3 * jax.random.normal(part_keys[3], (HID_WAYS, d_shard), jnp.float32))
    residual = (noise * row_scale * block_scale * col_scale).reshape(TOKENS, D_MODEL)
    gain_mlp = jax.random.uniform(keys[1], (D_MODEL,), jnp.float32, minval=0.5, maxval=1.5)
    gain_attn = jax.random.uniform(keys[2], (D_MODEL,), jnp.float32, minval=0.5, maxval=1.5)
    w_gate = jax.random.normal(keys[3], (D_MODEL, D_FF), jnp.float32) * D_MODEL ** -0.5
    w_up = jax.random.normal(keys[4], (D_MODEL, D_FF), jnp.float32) * D_MODEL ** -0.5
    w_down = jax.random.normal(keys[5], (D_FF, D_MODEL), jnp.float32) * (2.0 * D_FF ** -0.5)
    w_qkv = jax.random.normal(keys[6], (D_MODEL, QKV_DIM), jnp.float32) * D_MODEL ** -0.5
    return dict(residual=residual.astype(jnp.bfloat16), gain_mlp=gain_mlp, gain_attn=gain_attn,
                w_gate=w_gate.astype(jnp.bfloat16), w_up=w_up.astype(jnp.bfloat16),
                w_down=w_down.astype(jnp.bfloat16), w_qkv=w_qkv.astype(jnp.bfloat16))


def rms_norm(resid_rows, gain):
    resid32 = resid_rows.astype(jnp.float32)
    sum_sq = jnp.sum(resid32 * resid32, axis=1, keepdims=True)
    scale = lax.rsqrt(sum_sq / resid_rows.shape[1] + NORM_EPS)
    return (resid32 * scale * gain[None, :]).astype(jnp.bfloat16)


def block_sum(left_mat, right_mat, ways):
    row_count = left_mat.shape[0]
    inner_dim = left_mat.shape[1] // ways
    left_blocks = jnp.transpose(left_mat.reshape(row_count, ways, inner_dim), (1, 0, 2))
    right_blocks = right_mat.reshape(ways, inner_dim, right_mat.shape[1])

    def add_piece(running, pair):
        piece = jnp.dot(pair[0], pair[1], preferred_element_type=jnp.float32).astype(jnp.bfloat16)
        return running + piece.astype(jnp.float32), None

    start_sum = jnp.zeros((row_count, right_mat.shape[1]), jnp.float32)
    summed, _ = lax.scan(add_piece, start_sum, (left_blocks, right_blocks))
    return summed.astype(jnp.bfloat16)


def reference(residual, gain_mlp, gain_attn, w_gate, w_up, w_down, w_qkv):
    normed = rms_norm(residual, gain_mlp)
    gate_sum = block_sum(normed, w_gate, HID_WAYS)
    up_sum = block_sum(normed, w_up, HID_WAYS)
    hidden_act = (jax.nn.silu(gate_sum.astype(jnp.float32)) * up_sum.astype(jnp.float32)).astype(jnp.bfloat16)
    down_sum = block_sum(hidden_act, w_down, FFN_WAYS)
    residual_out = (residual.astype(jnp.float32) + down_sum.astype(jnp.float32)).astype(jnp.bfloat16)
    normed_next = rms_norm(residual_out, gain_attn)
    qkv_out = block_sum(normed_next, w_qkv, HID_WAYS)
    return (residual_out, qkv_out)
```

```python
import functools

import jax
import jax.numpy as jnp
from jax import lax
from jax.experimental import pallas as pl
from jax.experimental.pallas import tpu as pltpu
from jax.sharding import PartitionSpec as P

NORM_EPS = 1e-6
MESH = pl.DeviceIdType.MESH
N_CHUNK = 4
Q_CHUNK = 2


class Ring:
    def __init__(self, me, dev, slot, send, recv):
        self.me, self.dev, self.slot, self.send, self.recv = me, dev, slot, send, recv
        self.right, self.left, self.far = (lax.rem(me + d, 4) for d in (1, 3, 2))

    def copy(self, k, n, owner, half, target, src=None):
        dst = self.slot(k, owner, half)
        return pltpu.make_async_remote_copy(
            src_ref=dst if src is None else src, dst_ref=dst,
            send_sem=self.send.at[k, n], recv_sem=self.recv.at[k, n],
            device_id=self.dev(target), device_id_type=MESH)

    def start_own(self, k, src=None):
        for n, half, target in ((0, 0, self.right), (3, 1, self.left), (1, 1, self.right), (4, 0, self.left)):
            self.copy(k, n, self.me, half, target, None if src is None else src(k, half)).start()

    def forward(self, k):
        self.copy(k, 0, self.left, 0, self.right).wait_recv()
        self.copy(k, 2, self.left, 0, self.right).start()
        self.copy(k, 3, self.right, 1, self.left).wait_recv()
        self.copy(k, 5, self.right, 1, self.left).start()

    def wait_left(self, k):
        self.copy(k, 1, self.left, 1, self.right).wait_recv()

    def wait_right(self, k):
        self.copy(k, 4, self.right, 0, self.left).wait_recv()

    def wait_far(self, k):
        self.copy(k, 2, self.far, 0, self.right).wait_recv()
        self.copy(k, 5, self.far, 1, self.left).wait_recv()

    def finish(self, k):
        self.wait_left(k)
        self.wait_right(k)
        self.wait_far(k)

    def drain(self, k):
        for n, owner, half, target in ((0, self.me, 0, self.right), (1, self.me, 1, self.right),
                                       (2, self.left, 0, self.right), (3, self.me, 1, self.left),
                                       (4, self.me, 0, self.left), (5, self.right, 1, self.left)):
            self.copy(k, n, owner, half, target).wait_send()


def kernel(d_model, x, gains, w_gate, w_up, w_down, w_qkv,
           x2_out, qkv_out, n_all, wq_all,
           xg, n_own, n_in, w_in, stage, act, wd_in, part, got, q_stage, gain_buf,
           loc, one_s, one_r, gain_s, gain_r, xd_s, xd_r, wx_s, wx_r, wd_s, wd_r, wq_s, wq_r, wqd_s, wqd_r,
           rs_s, rs_r, qy_s, qy_r, qd_s, qd_r,
           xr_s, xr_r, nr_s, nr_r, ar_s, ar_r, wr_s, wr_r, x2r_s, x2r_r, or_s, or_r, qr_s, qr_r):
    hid, row = lax.axis_index('hid'), lax.axis_index('ffn')
    chip, core = lax.div(hid, 2), lax.rem(hid, 2)
    mate = hid + 1 - 2 * core
    right, left, far = (lax.rem(chip + d, 4) for d in (1, 3, 2))
    tokens, width = x.shape
    half_t, block = tokens // 2, tokens // 8
    sub = block // 2
    ff = w_gate.shape[1] // 4
    qb = w_qkv.shape[1] // 4
    nc, qc = block // N_CHUNK, block // Q_CHUNK

    def dev_x(c):
        return {'hid': 2 * c + core, 'ffn': row}

    def dev_y(r):
        return {'hid': hid, 'ffn': r}

    mate_dev = {'hid': mate, 'ffn': row}

    def remote(src, dst, s, r, dev):
        return pltpu.make_async_remote_copy(src_ref=src, dst_ref=dst, send_sem=s, recv_sem=r,
                                            device_id=dev, device_id_type=MESH)

    def local(src, dst, n):
        return pltpu.make_async_copy(src, dst, loc.at[n])

    def rows_of(c, r):
        return c * half_t + r * block

    def ds(start, size):
        return pl.ds(pl.multiple_of(start, size), size)

    barrier = pltpu.get_barrier_semaphore()
    for d in range(1, 8):
        pl.semaphore_signal(barrier, inc=1, device_id={'hid': lax.rem(hid + d, 8), 'ffn': row}, device_id_type=MESH)
    for d in range(1, 4):
        pl.semaphore_signal(barrier, inc=1, device_id=dev_y(lax.rem(row + d, 4)), device_id_type=MESH)
    pl.semaphore_wait(barrier, 10)

    def x_chunk(k, c):
        return x.at[ds(rows_of(c, row) + k * nc, nc), :]

    def xd(k, h, c):
        return remote(x_chunk(k, c), xg.at[h, k * nc:(k + 1) * nc, :], xd_s.at[k], xd_r.at[k], mate_dev)

    x_own = [local(x_chunk(k, core), xg.at[hid, k * nc:(k + 1) * nc, :], k) for k in range(N_CHUNK)]
    for k in range(N_CHUNK):
        xd(k, hid, 1 - core).start()
        x_own[k].start()

    def gain_copy(d):
        to = lax.rem(hid + d, 8)
        return remote(gains, gain_buf.at[hid], gain_s.at[d - 1], gain_r.at[d - 1], {'hid': to, 'ffn': row})

    def gain_got(d):
        src = lax.rem(hid + 8 - d, 8)
        return remote(gains, gain_buf.at[src], gain_s.at[d - 1], gain_r.at[d - 1], {'hid': src, 'ffn': row})

    for d in range(1, 8):
        gain_copy(d).start()
    gain_own = local(gains, gain_buf.at[hid], 4)
    gain_own.start()

    x_ring = Ring(chip, dev_x, lambda k, c, h: xg.at[2 * c + h, k * nc:(k + 1) * nc, :], xr_s, xr_r)
    for k in range(N_CHUNK):
        x_own[k].wait()
        xd(k, mate, core).wait_recv()
        x_ring.start_own(k)

    mats = (w_gate, w_up)

    def cols(m, c):
        return mats[m].at[:, ds(c * ff, ff)]

    def w_rows(m, h):
        return w_in.at[ds(h * width, width), m * ff:(m + 1) * ff]

    w_own = [local(cols(m, chip), w_rows(m, hid), 5 + m) for m in range(2)]
    wd_own = local(w_down, wd_in.at[core], 7)
    for c in (*w_own, wd_own):
        c.start()
    wd_mate = remote(w_down, wd_in.at[core], one_s.at[0], one_r.at[0], mate_dev)
    wd_mate.start()

    def w_mate(n, m, h):
        return remote(w_rows(m, h), w_rows(m, h), wd_s.at[n, m], wd_r.at[n, m], mate_dev)

    for m in range(2):
        remote(cols(m, chip), w_rows(m, hid), wd_s.at[0, m], wd_r.at[0, m], mate_dev).start()

    for k in range(N_CHUNK):
        x_ring.forward(k)

    hw = width // 2

    def far_half(m, side, c):
        return mats[m].at[side * hw:(side + 1) * hw, ds(c * ff, ff)]

    def half_rows(m, h, side):
        return w_in.at[ds(h * width + side * hw, hw), m * ff:(m + 1) * ff]

    for m in range(2):
        remote(far_half(m, 0, far), stage.at[0, m], wx_s.at[0, m], wx_r.at[0, m], dev_x(right)).start()
        remote(far_half(m, 1, far), stage.at[1, m], wx_s.at[1, m], wx_r.at[1, m], dev_x(left)).start()
    for m in range(2):
        remote(cols(m, right), w_rows(m, hid), wx_s.at[2, m], wx_r.at[2, m], dev_x(right)).start()
        remote(cols(m, left), w_rows(m, hid), wx_s.at[3, m], wx_r.at[3, m], dev_x(left)).start()

    wq_in = local(w_qkv.at[:, ds(chip * qb, qb)], q_stage.at[0:width, 0:qb], 8)
    wq_in.start()
    for n, c in enumerate((right, left, far)):
        remote(w_qkv.at[:, ds(c * qb, qb)], wq_all.at[row, core, chip], wq_s.at[n], wq_r.at[n], dev_x(c)).start()

    n_ring = Ring(row, dev_y, lambda k, r, h: n_all.at[r, k * nc + h * (nc // 2):k * nc + (h + 1) * (nc // 2), :],
                  nr_s, nr_r)

    def n_src(k, h):
        return n_own.at[k * nc + h * (nc // 2):k * nc + (h + 1) * (nc // 2), :]

    def norm(start, count, which):
        tile = min(16, count)

        def body(t, carry):
            rows = ds(start + t * tile, tile)
            total = jnp.zeros((tile, 1), jnp.float32)
            for h in range(8):
                piece = xg[h, rows, :].astype(jnp.float32)
                total += jnp.sum(piece * piece, axis=1, keepdims=True)
            scale = lax.rsqrt(total / d_model + NORM_EPS)
            for h in range(8):
                piece = xg[h, rows, :].astype(jnp.float32)
                n_own[rows, h * width:(h + 1) * width] = (
                    piece * scale * gain_buf[h, which:which + 1, :]).astype(n_own.dtype)
            return carry

        lax.fori_loop(0, count // tile, body, 0)

    gain_own.wait()
    for d in range(1, 8):
        gain_got(d).wait_recv()
    n_keep = [local(n_own.at[k * nc:(k + 1) * nc, :], n_all.at[row, k * nc:(k + 1) * nc, :], 9 + k)
              for k in range(N_CHUNK)]
    for k in range(N_CHUNK):
        x_ring.finish(k)
        norm(k * nc, nc, 0)
        n_ring.start_own(k, n_src)
        n_keep[k].start()

    wq_in.wait()
    wq_keep = local(q_stage.at[0:width, 0:qb], wq_all.at[row, core, chip], 8)
    wq_keep.start()

    n_ring.forward(0)
    for m in range(2):
        remote(stage.at[0, m], stage.at[0, m], wx_s.at[0, m], wx_r.at[0, m], dev_x(right)).wait_recv()
        remote(stage.at[0, m], half_rows(m, 2 * left + core, 0), wx_s.at[4, m], wx_r.at[4, m], dev_x(right)).start()
        remote(stage.at[1, m], stage.at[1, m], wx_s.at[1, m], wx_r.at[1, m], dev_x(left)).wait_recv()
        remote(stage.at[1, m], half_rows(m, 2 * right + core, 1), wx_s.at[5, m], wx_r.at[5, m], dev_x(left)).start()
    n_ring.forward(1)
    n_ring.forward(2)
    for m in range(2):
        remote(w_rows(m, hid), w_rows(m, 2 * left + core), wx_s.at[2, m], wx_r.at[2, m], dev_x(right)).wait_recv()
        w_mate(1, m, 2 * left + core).start()
        remote(w_rows(m, hid), w_rows(m, 2 * right + core), wx_s.at[3, m], wx_r.at[3, m], dev_x(left)).wait_recv()
        w_mate(2, m, 2 * right + core).start()
    n_ring.forward(3)
    for m in range(2):
        h = 2 * far + core
        remote(stage.at[0, m], half_rows(m, h, 0), wx_s.at[4, m], wx_r.at[4, m], dev_x(right)).wait_recv()
        remote(stage.at[1, m], half_rows(m, h, 1), wx_s.at[5, m], wx_r.at[5, m], dev_x(left)).wait_recv()
        w_mate(3, m, h).start()
    wq_keep.wait()
    for n, c in enumerate((left, right, far)):
        remote(w_qkv.at[:, ds(c * qb, qb)], wq_all.at[row, core, c], wq_s.at[n], wq_r.at[n], dev_x(c)).wait_recv()
    wq_ring = Ring(row, dev_y, lambda k, r, h: wq_all.at[r, core, 2 * h:2 * h + 2], wr_s, wr_r)
    for c in w_own:
        c.wait()
    for m in range(2):
        for n, c in enumerate((chip, left, right, far)):
            w_mate(n, m, 2 * c + 1 - core).wait_recv()
    wd_own.wait()
    remote(w_down, wd_in.at[1 - core], one_s.at[0], one_r.at[0], mate_dev).wait_recv()
    for k in range(N_CHUNK):
        n_keep[k].wait()
        x_ring.drain(k)

    a_ring = Ring(chip, dev_x, lambda s, c, h: act.at[s, h * (sub // 2):(h + 1) * (sub // 2), ds(c * ff, ff)],
                  ar_s, ar_r)

    def n_load(s):
        r = lax.rem(row + lax.div(s, 2) + 1, 4)
        return local(n_all.at[r, ds(lax.rem(s, 2) * sub, sub), :], n_in, 13)

    def part_copy(s, back):
        d = lax.div(s, 2) + 1
        to = lax.rem(row + d, 4)
        return remote(part.at[s], got.at[s], rs_s.at[s], rs_r.at[s], dev_y(to))

    for k in range(N_CHUNK):
        n_ring.wait_right(k)
    n_load(0).start()

    def step(s, carry):
        @pl.when(s < 8)
        def _():
            n_load(s).wait()
            gate = jnp.dot(n_in[...], w_in[:, 0:ff], preferred_element_type=jnp.float32).astype(jnp.bfloat16)
            up = jnp.dot(n_in[...], w_in[:, ff:2 * ff], preferred_element_type=jnp.float32).astype(jnp.bfloat16)
            act[s, :, ds(chip * ff, ff)] = (
                jax.nn.silu(gate.astype(jnp.float32)) * up.astype(jnp.float32)).astype(act.dtype)
            a_ring.start_own(s)

        @pl.when((s >= 1) & (s < 9))
        def _():
            a_ring.forward(s - 1)

        @pl.when(s == 1)
        def _():
            for k in range(N_CHUNK):
                n_ring.wait_far(k)

        @pl.when(s == 3)
        def _():
            for k in range(N_CHUNK):
                n_ring.wait_left(k)
            wq_ring.start_own(0)

        @pl.when(s == 6)
        def _():
            wq_ring.forward(0)

        @pl.when(s < 7)
        def _():
            n_load(s + 1).start()

        @pl.when(s >= 2)
        def _():
            b = s - 2
            a_ring.finish(b)
            for c in range(2):
                part[b, c] = jnp.dot(act[b], wd_in[c], preferred_element_type=jnp.float32).astype(part.dtype)

            @pl.when(b < 6)
            def _():
                part_copy(b, 0).start()

        return carry

    lax.fori_loop(0, 10, step, 0)

    wq_ring.finish(0)
    for r in range(4):
        remote(wq_all.at[r, core], wq_all.at[r, core], wqd_s.at[r], wqd_r.at[r], mate_dev).start()

    for s in range(6):
        part_copy(s, 0).wait_recv()
    for k in range(N_CHUNK):
        n_ring.drain(k)
    tile = min(16, sub)
    for s in range(2):
        def add(t, carry):
            rows = ds(t * tile, tile)
            out_rows = ds(s * sub + t * tile, tile)
            for c in range(2):
                down = part[6 + s, c, rows, :].astype(jnp.float32)
                for q in range(3):
                    down += got[2 * q + s, c, rows, :].astype(jnp.float32)
                old = xg[2 * chip + c, out_rows, :].astype(jnp.float32)
                xg[2 * chip + c, out_rows, :] = (
                    old + down.astype(jnp.bfloat16).astype(jnp.float32)).astype(xg.dtype)
            return carry

        lax.fori_loop(0, sub // tile, add, 0)

    x2_ring = Ring(chip, dev_x, lambda k, c, h: xg.at[2 * c + h, k * qc:(k + 1) * qc, :], x2r_s, x2r_r)
    for k in range(Q_CHUNK):
        x2_ring.start_own(k)

    def x2_rows(c, r):
        return x2_out.at[ds(rows_of(c, r), block), :]

    x2_keep = local(xg.at[hid], x2_rows(core, row), 0)
    x2_keep.start()
    x2_mate = remote(xg.at[mate], x2_rows(core, row), one_s.at[1], one_r.at[1], mate_dev)
    x2_mate.start()

    for r in range(4):
        remote(wq_all.at[r, 1 - core], wq_all.at[r, 1 - core], wqd_s.at[r], wqd_r.at[r], mate_dev).wait_recv()

    def wq_load(r, c, i):
        return local(wq_all.at[r, c, i], w_in.at[(2 * i + c) * width:(2 * i + c + 1) * width, r * qb:(r + 1) * qb],
                     16 + r * 8 + c * 4 + i)

    wq_loads = [wq_load(r, c, i) for r in range(4) for c in range(2) for i in range(4)]
    for m in range(2):
        for n in range(4):
            w_mate(n, m, hid).wait_send()
    for c in wq_loads:
        c.start()

    for k in range(Q_CHUNK):
        x2_ring.forward(k)
    x2_keep.wait()
    remote(xg.at[mate], x2_rows(1 - core, row), one_s.at[1], one_r.at[1], mate_dev).wait_recv()
    out_ring = Ring(row, dev_y, lambda k, r, h: x2_rows(h, r), or_s, or_r)
    out_ring.start_own(0)
    for c in wq_loads:
        c.wait()

    def q_rows(r, start, count):
        return ds(rows_of(core, r) + start, count)

    def qy(k, n, r):
        return remote(q_stage.at[k * qc:(k + 1) * qc, ds(r * qb, qb)],
                      qkv_out.at[q_rows(row, k * qc, qc), ds(chip * qb, qb)],
                      qy_s.at[k, n], qy_r.at[k, n], dev_y(r))

    def qy_got(k, n, r):
        return remote(q_stage.at[k * qc:(k + 1) * qc, ds(r * qb, qb)],
                      qkv_out.at[q_rows(r, k * qc, qc), ds(chip * qb, qb)],
                      qy_s.at[k, n], qy_r.at[k, n], dev_y(r))

    q_keep = [local(q_stage.at[k * qc:(k + 1) * qc, ds(row * qb, qb)],
                    qkv_out.at[q_rows(row, k * qc, qc), ds(chip * qb, qb)], 1 + k) for k in range(Q_CHUNK)]
    for k in range(Q_CHUNK):
        x2_ring.finish(k)
        norm(k * qc, qc, 1)
        q_stage[k * qc:(k + 1) * qc, :] = jnp.dot(
            n_own[k * qc:(k + 1) * qc, :], w_in[:, 0:4 * qb], preferred_element_type=jnp.float32).astype(q_stage.dtype)
        for n in range(3):
            qy(k, n, lax.rem(row + n + 1, 4)).start()
        q_keep[k].start()
    out_ring.forward(0)

    q_ring = Ring(chip, dev_x,
                  lambda n, c, h: qkv_out.at[ds(rows_of(core, lax.rem(row + 4 - n, 4)) + h * sub, sub), ds(c * qb, qb)],
                  qr_s, qr_r)

    def q_mate(n, c):
        rows = ds(rows_of(c, lax.rem(row + 4 - n, 4)), block)
        return remote(qkv_out.at[rows, :], qkv_out.at[rows, :], qd_s.at[n], qd_r.at[n], mate_dev)

    for c in q_keep:
        c.wait()
    q_ring.start_own(0)
    for n in range(1, 4):
        for k in range(Q_CHUNK):
            qy_got(k, n - 1, lax.rem(row + 4 - n, 4)).wait_recv()
        q_ring.start_own(n)
        q_ring.forward(n - 1)
        if n >= 2:
            q_ring.finish(n - 2)
            q_mate(n - 2, core).start()
    q_ring.forward(3)
    for n in (2, 3):
        q_ring.finish(n)
        q_mate(n, core).start()
    out_ring.finish(0)

    for n in range(4):
        q_mate(n, 1 - core).wait_recv()
    for d in range(1, 8):
        gain_copy(d).wait_send()
    for k in range(N_CHUNK):
        xd(k, hid, 1 - core).wait_send()
    wd_mate.wait_send()
    x2_mate.wait_send()
    for m in range(2):
        for n in range(6):
            remote(stage.at[0, m] if n in (0, 1, 4, 5) else w_rows(m, hid),
                   stage.at[0, m] if n in (0, 1, 4, 5) else w_rows(m, hid),
                   wx_s.at[n, m], wx_r.at[n, m], dev_x(right)).wait_send()
    for n in range(3):
        remote(wq_all.at[row, core, chip], wq_all.at[row, core, chip], wq_s.at[n], wq_r.at[n],
               dev_x(right)).wait_send()
    for r in range(4):
        remote(wq_all.at[r, core], wq_all.at[r, core], wqd_s.at[r], wqd_r.at[r], mate_dev).wait_send()
    for s in range(6):
        part_copy(s, 0).wait_send()
    for k in range(Q_CHUNK):
        for n in range(3):
            qy(k, n, lax.rem(row + n + 1, 4)).wait_send()
        x2_ring.drain(k)
    for n in range(4):
        q_mate(n, core).wait_send()
        q_ring.drain(n)

    def drain_act(s, carry):
        a_ring.drain(s)
        return carry

    lax.fori_loop(0, 8, drain_act, 0)
    wq_ring.drain(0)
    out_ring.drain(0)


def solution(mesh):
    hid_ways, ffn_ways = mesh.shape['hid'], mesh.shape['ffn']
    assert hid_ways == 8 and ffn_ways == 4

    def device_step(residual, gain_mlp, gain_attn, w_gate, w_up, w_down, w_qkv):
        tokens, width = residual.shape
        d_model = width * hid_ways
        block, sub = tokens // 8, tokens // 16
        ff, qb = w_gate.shape[1] // 4, w_qkv.shape[1] // 4
        gains = jnp.stack([gain_mlp, gain_attn])
        dtype = residual.dtype
        any_spec = pl.BlockSpec(memory_space=pl.ANY)
        dma = pltpu.SemaphoreType.DMA
        outs = pl.pallas_call(
            functools.partial(kernel, d_model),
            out_shape=(jax.ShapeDtypeStruct((tokens, width), dtype),
                       jax.ShapeDtypeStruct((tokens, w_qkv.shape[1]), dtype),
                       jax.ShapeDtypeStruct((4, block, d_model), dtype),
                       jax.ShapeDtypeStruct((4, 2, 4, width, qb), dtype)),
            in_specs=[any_spec] * 6,
            out_specs=(any_spec,) * 4,
            scratch_shapes=[
                pltpu.VMEM((8, block, width), dtype),
                pltpu.VMEM((block, d_model), dtype),
                pltpu.VMEM((sub, d_model), dtype),
                pltpu.VMEM((d_model, 2 * ff), dtype),
                pltpu.VMEM((2, 2, width // 2, ff), dtype),
                pltpu.VMEM((8, sub, 4 * ff), dtype),
                pltpu.VMEM((2, 4 * ff, width), dtype),
                pltpu.VMEM((8, 2, sub, width), dtype),
                pltpu.VMEM((6, 2, sub, width), dtype),
                pltpu.VMEM((max(block, width), 4 * qb), dtype),
                pltpu.VMEM((8, 2, width), jnp.float32),
                dma((48,)), dma((2,)), dma((2,)), dma((7,)), dma((7,)),
                dma((N_CHUNK,)), dma((N_CHUNK,)), dma((6, 2)), dma((6, 2)), dma((4, 2)), dma((4, 2)),
                dma((3,)), dma((3,)), dma((4,)), dma((4,)), dma((6,)), dma((6,)),
                dma((Q_CHUNK, 3)), dma((Q_CHUNK, 3)), dma((4,)), dma((4,)),
                dma((N_CHUNK, 6)), dma((N_CHUNK, 6)), dma((N_CHUNK, 6)), dma((N_CHUNK, 6)),
                dma((8, 6)), dma((8, 6)), dma((1, 6)), dma((1, 6)), dma((Q_CHUNK, 6)), dma((Q_CHUNK, 6)),
                dma((1, 6)), dma((1, 6)), dma((4, 6)), dma((4, 6)),
            ],
            compiler_params=pltpu.CompilerParams(
                collective_id=0, has_side_effects=True, vmem_limit_bytes=67043328),
            name='layer',
        )(residual, gains, w_gate, w_up, w_down, w_qkv)
        return outs[0], outs[1]

    return jax.shard_map(
        device_step, mesh=mesh,
        in_specs=(P('data', 'hid'), P('hid'), P('hid'), P('hid', 'ffn'), P('hid', 'ffn'),
                  P('ffn', 'hid'), P('hid', 'ffn')),
        out_specs=(P('data', 'hid'), P('data', 'ffn')),
        check_vma=False)
```

```python
import functools

import jax
import jax.numpy as jnp
from jax import lax
from jax.experimental import pallas as pl
from jax.experimental.pallas import tpu as pltpu
from jax.sharding import PartitionSpec as P

NORM_EPS = 1e-6
MESH = pl.DeviceIdType.MESH
N_CHUNK = 4
Q_CHUNK = 2


class Ring:
    def __init__(self, me, dev, slot, send, recv):
        self.me, self.dev, self.slot, self.send, self.recv = me, dev, slot, send, recv
        self.right, self.left, self.far = (lax.rem(me + d, 4) for d in (1, 3, 2))

    def copy(self, k, n, owner, half, target, src=None):
        dst = self.slot(k, owner, half)
        return pltpu.make_async_remote_copy(
            src_ref=dst if src is None else src, dst_ref=dst,
            send_sem=self.send.at[k, n], recv_sem=self.recv.at[k, n],
            device_id=self.dev(target), device_id_type=MESH)

    def start_own(self, k, src=None, order=(0, 3, 1, 4)):
        for n in order:
            half, target = ((0, self.right), (1, self.right), None, (1, self.left), (0, self.left))[n]
            self.copy(k, n, self.me, half, target, None if src is None else src(k, half)).start()

    def forward(self, k):
        self.copy(k, 0, self.left, 0, self.right).wait_recv()
        self.copy(k, 2, self.left, 0, self.right).start()
        self.copy(k, 3, self.right, 1, self.left).wait_recv()
        self.copy(k, 5, self.right, 1, self.left).start()

    def wait_left(self, k):
        self.copy(k, 1, self.left, 1, self.right).wait_recv()

    def wait_right(self, k):
        self.copy(k, 4, self.right, 0, self.left).wait_recv()

    def wait_far(self, k):
        self.copy(k, 2, self.far, 0, self.right).wait_recv()
        self.copy(k, 5, self.far, 1, self.left).wait_recv()

    def finish(self, k):
        self.wait_left(k)
        self.wait_right(k)
        self.wait_far(k)

    def drain(self, k):
        for n, owner, half, target in ((0, self.me, 0, self.right), (1, self.me, 1, self.right),
                                       (2, self.left, 0, self.right), (3, self.me, 1, self.left),
                                       (4, self.me, 0, self.left), (5, self.right, 1, self.left)):
            self.copy(k, n, owner, half, target).wait_send()


def kernel(d_model, x, gains, w_gate, w_up, w_down, w_qkv,
           x2_out, qkv_out, n_all, wq_all,
           xg, n_own, n_in, w_in, stage, act, wd_in, part, got, q_stage, gain_buf,
           loc, one_s, one_r, gain_s, gain_r, xd_s, xd_r, wx_s, wx_r, wd_s, wd_r, wq_s, wq_r, wqd_s, wqd_r,
           rs_s, rs_r, qy_s, qy_r, qd_s, qd_r,
           xr_s, xr_r, nr_s, nr_r, ar_s, ar_r, wr_s, wr_r, x2r_s, x2r_r, or_s, or_r, qr_s, qr_r):
    hid, row = lax.axis_index('hid'), lax.axis_index('ffn')
    chip, core = lax.div(hid, 2), lax.rem(hid, 2)
    mate = hid + 1 - 2 * core
    right, left, far = (lax.rem(chip + d, 4) for d in (1, 3, 2))
    tokens, width = x.shape
    half_t, block = tokens // 2, tokens // 8
    sub = block // 2
    ff = w_gate.shape[1] // 4
    qb = w_qkv.shape[1] // 4
    nc, qc = block // N_CHUNK, block // Q_CHUNK

    def dev_x(c):
        return {'hid': 2 * c + core, 'ffn': row}

    def dev_y(r):
        return {'hid': hid, 'ffn': r}

    mate_dev = {'hid': mate, 'ffn': row}

    def remote(src, dst, s, r, dev):
        return pltpu.make_async_remote_copy(src_ref=src, dst_ref=dst, send_sem=s, recv_sem=r,
                                            device_id=dev, device_id_type=MESH)

    def local(src, dst, n):
        return pltpu.make_async_copy(src, dst, loc.at[n])

    def rows_of(c, r):
        return c * half_t + r * block

    def ds(start, size):
        return pl.ds(pl.multiple_of(start, size), size)

    barrier = pltpu.get_barrier_semaphore()
    for d in range(1, 8):
        pl.semaphore_signal(barrier, inc=1, device_id={'hid': lax.rem(hid + d, 8), 'ffn': row}, device_id_type=MESH)
    for d in range(1, 4):
        pl.semaphore_signal(barrier, inc=1, device_id=dev_y(lax.rem(row + d, 4)), device_id_type=MESH)
    pl.semaphore_wait(barrier, 10)

    def x_chunk(k, c):
        return x.at[ds(rows_of(c, row) + k * nc, nc), :]

    def xd(k, h, c):
        return remote(x_chunk(k, c), xg.at[h, k * nc:(k + 1) * nc, :], xd_s.at[k], xd_r.at[k], mate_dev)

    x_own = [local(x_chunk(k, core), xg.at[hid, k * nc:(k + 1) * nc, :], k) for k in range(N_CHUNK)]
    for k in range(N_CHUNK):
        xd(k, hid, 1 - core).start()
        x_own[k].start()

    def gain_copy(d):
        to = lax.rem(hid + d, 8)
        return remote(gains, gain_buf.at[hid], gain_s.at[d - 1], gain_r.at[d - 1], {'hid': to, 'ffn': row})

    def gain_got(d):
        src = lax.rem(hid + 8 - d, 8)
        return remote(gains, gain_buf.at[src], gain_s.at[d - 1], gain_r.at[d - 1], {'hid': src, 'ffn': row})

    for d in range(1, 8):
        gain_copy(d).start()
    gain_own = local(gains, gain_buf.at[hid], 4)
    gain_own.start()

    x_ring = Ring(chip, dev_x, lambda k, c, h: xg.at[2 * c + (core if h == 0 else 1 - core), k * nc:(k + 1) * nc, :],
                  xr_s, xr_r)
    for k in range(N_CHUNK):
        x_ring.start_own(k, lambda k, h: x_chunk(k, core), order=(0, 4))
        xd(k, mate, core).wait_recv()
        x_ring.start_own(k, order=(3, 1))
    for k in range(N_CHUNK):
        x_own[k].wait()

    mats = (w_gate, w_up)

    def cols(m, c):
        return mats[m].at[:, ds(c * ff, ff)]

    def w_rows(m, h):
        return w_in.at[ds(h * width, width), m * ff:(m + 1) * ff]

    w_own = [local(cols(m, chip), w_rows(m, hid), 5 + m) for m in range(2)]
    wd_own = local(w_down, wd_in.at[core], 7)
    for c in (*w_own, wd_own):
        c.start()
    wd_mate = remote(w_down, wd_in.at[core], one_s.at[0], one_r.at[0], mate_dev)
    wd_mate.start()

    def w_mate(n, m, h):
        return remote(w_rows(m, h), w_rows(m, h), wd_s.at[n, m], wd_r.at[n, m], mate_dev)

    for m in range(2):
        remote(cols(m, chip), w_rows(m, hid), wd_s.at[0, m], wd_r.at[0, m], mate_dev).start()

    for k in range(N_CHUNK):
        x_ring.forward(k)

    hw = width // 2

    def far_half(m, side, c):
        return mats[m].at[side * hw:(side + 1) * hw, ds(c * ff, ff)]

    def half_rows(m, h, side):
        return w_in.at[ds(h * width + side * hw, hw), m * ff:(m + 1) * ff]

    for m in range(2):
        remote(far_half(m, 0, far), stage.at[0, m], wx_s.at[0, m], wx_r.at[0, m], dev_x(right)).start()
        remote(far_half(m, 1, far), stage.at[1, m], wx_s.at[1, m], wx_r.at[1, m], dev_x(left)).start()
    for m in range(2):
        remote(cols(m, right), w_rows(m, hid), wx_s.at[2, m], wx_r.at[2, m], dev_x(right)).start()
        remote(cols(m, left), w_rows(m, hid), wx_s.at[3, m], wx_r.at[3, m], dev_x(left)).start()

    wq_in = local(w_qkv.at[:, ds(chip * qb, qb)], q_stage.at[0:width, 0:qb], 8)
    wq_in.start()
    via, back = lax.rem(chip + 1 + 2 * core, 4), lax.rem(chip + 3 - 2 * core, 4)
    wq_tmp = q_stage.at[0:width, qb:2 * qb]

    def wq_copy(n, src, owner, c):
        return remote(src, wq_tmp if n == 2 else wq_all.at[row, core, owner], wq_s.at[n], wq_r.at[n], dev_x(c))

    n_ring = Ring(row, dev_y, lambda k, r, h: n_all.at[r, k * nc + h * (nc // 2):k * nc + (h + 1) * (nc // 2), :],
                  nr_s, nr_r)

    def n_src(k, h):
        return n_own.at[k * nc + h * (nc // 2):k * nc + (h + 1) * (nc // 2), :]

    def norm(start, count, which):
        tile = min(16, count)

        def body(t, carry):
            rows = ds(start + t * tile, tile)
            total = jnp.zeros((tile, 1), jnp.float32)
            for h in range(8):
                piece = xg[h, rows, :].astype(jnp.float32)
                total += jnp.sum(piece * piece, axis=1, keepdims=True)
            scale = lax.rsqrt(total / d_model + NORM_EPS)
            for h in range(8):
                piece = xg[h, rows, :].astype(jnp.float32)
                n_own[rows, h * width:(h + 1) * width] = (
                    piece * scale * gain_buf[h, which:which + 1, :]).astype(n_own.dtype)
            return carry

        lax.fori_loop(0, count // tile, body, 0)

    gain_own.wait()
    for d in range(1, 8):
        gain_got(d).wait_recv()
    n_keep = [local(n_own.at[k * nc:(k + 1) * nc, :], n_all.at[row, k * nc:(k + 1) * nc, :], 9 + k)
              for k in range(N_CHUNK)]
    for k in range(N_CHUNK):
        x_ring.finish(k)
        norm(k * nc, nc, 0)
        n_ring.start_own(k, n_src)
        n_keep[k].start()

    wq_in.wait()
    wq_keep = local(q_stage.at[0:width, 0:qb], wq_all.at[row, core, chip], 8)
    wq_keep.start()

    n_ring.forward(0)
    for m in range(2):
        remote(stage.at[0, m], stage.at[0, m], wx_s.at[0, m], wx_r.at[0, m], dev_x(right)).wait_recv()
        remote(stage.at[0, m], half_rows(m, 2 * left + core, 0), wx_s.at[4, m], wx_r.at[4, m], dev_x(right)).start()
        remote(stage.at[1, m], stage.at[1, m], wx_s.at[1, m], wx_r.at[1, m], dev_x(left)).wait_recv()
        remote(stage.at[1, m], half_rows(m, 2 * right + core, 1), wx_s.at[5, m], wx_r.at[5, m], dev_x(left)).start()
    wq_copy(2, w_qkv.at[:, ds(far * qb, qb)], chip, via).start()
    wq_copy(0, w_qkv.at[:, ds(right * qb, qb)], chip, right).start()
    wq_copy(1, w_qkv.at[:, ds(left * qb, qb)], chip, left).start()
    n_ring.forward(1)
    n_ring.forward(2)
    for m in range(2):
        remote(w_rows(m, hid), w_rows(m, 2 * left + core), wx_s.at[2, m], wx_r.at[2, m], dev_x(right)).wait_recv()
        w_mate(1, m, 2 * left + core).start()
        remote(w_rows(m, hid), w_rows(m, 2 * right + core), wx_s.at[3, m], wx_r.at[3, m], dev_x(left)).wait_recv()
        w_mate(2, m, 2 * right + core).start()
    n_ring.forward(3)
    for m in range(2):
        h = 2 * far + core
        remote(stage.at[0, m], half_rows(m, h, 0), wx_s.at[4, m], wx_r.at[4, m], dev_x(right)).wait_recv()
        remote(stage.at[1, m], half_rows(m, h, 1), wx_s.at[5, m], wx_r.at[5, m], dev_x(left)).wait_recv()
        w_mate(3, m, h).start()
    wq_keep.wait()
    wq_ring = Ring(row, dev_y, lambda k, r, h: wq_all.at[r, core, 2 * h:2 * h + 2], wr_s, wr_r)
    for c in w_own:
        c.wait()
    for m in range(2):
        for n, c in enumerate((chip, left, right, far)):
            w_mate(n, m, 2 * c + 1 - core).wait_recv()
    wd_own.wait()
    remote(w_down, wd_in.at[1 - core], one_s.at[0], one_r.at[0], mate_dev).wait_recv()
    for k in range(N_CHUNK):
        n_keep[k].wait()
        x_ring.drain(k)

    a_ring = Ring(chip, dev_x, lambda s, c, h: act.at[s, h * (sub // 2):(h + 1) * (sub // 2), ds(c * ff, ff)],
                  ar_s, ar_r)

    def n_load(s):
        r = lax.rem(row + lax.div(s, 2) + 1, 4)
        return local(n_all.at[r, ds(lax.rem(s, 2) * sub, sub), :], n_in, 13)

    def part_copy(s):
        d = lax.div(s, 2) + 1
        to = lax.rem(row + d, 4)
        return remote(part.at[s], got.at[s], rs_s.at[s], rs_r.at[s], dev_y(to))

    for k in range(N_CHUNK):
        n_ring.wait_right(k)
    n_load(0).start()

    x2_ring = Ring(chip, dev_x, lambda k, c, h: xg.at[2 * c + h, k * qc:(k + 1) * qc, :], x2r_s, x2r_r)

    def add_residual(s):
        tile = min(16, sub)
        for q in range(3):
            part_copy(2 * q + s).wait_recv()

        def add(t, carry):
            rows = ds(t * tile, tile)
            out_rows = ds(s * sub + t * tile, tile)
            for c in range(2):
                down = part[6 + s, c, rows, :].astype(jnp.float32)
                for q in range(3):
                    down += got[2 * q + s, c, rows, :].astype(jnp.float32)
                old = xg[2 * chip + c, out_rows, :].astype(jnp.float32)
                xg[2 * chip + c, out_rows, :] = (
                    old + down.astype(jnp.bfloat16).astype(jnp.float32)).astype(xg.dtype)
            return carry

        lax.fori_loop(0, sub // tile, add, 0)

    def wq_mate(r, c):
        return remote(wq_all.at[r, c], wq_all.at[r, c], wqd_s.at[r], wqd_r.at[r], mate_dev)

    wq_loads = [local(wq_all.at[r, c, i], w_in.at[(2 * i + c) * width:(2 * i + c + 1) * width, r * qb:(r + 1) * qb],
                      16 + r * 8 + c * 4 + i) for r in range(4) for c in range(2) for i in range(4)]

    def step(s, carry):
        @pl.when(s < 8)
        def _():
            n_load(s).wait()
            gate = jnp.dot(n_in[...], w_in[:, 0:ff], preferred_element_type=jnp.float32).astype(jnp.bfloat16)
            up = jnp.dot(n_in[...], w_in[:, ff:2 * ff], preferred_element_type=jnp.float32).astype(jnp.bfloat16)
            act[s, :, ds(chip * ff, ff)] = (
                jax.nn.silu(gate.astype(jnp.float32)) * up.astype(jnp.float32)).astype(act.dtype)
            a_ring.start_own(s)

        @pl.when((s >= 1) & (s < 9))
        def _():
            a_ring.forward(s - 1)

        @pl.when(s == 1)
        def _():
            wq_copy(2, w_qkv.at[:, ds(far * qb, qb)], chip, via).wait_recv()
            wq_copy(3, wq_tmp, back, via).start()
            for k in range(N_CHUNK):
                n_ring.wait_far(k)

        @pl.when(s == 3)
        def _():
            for k in range(N_CHUNK):
                n_ring.wait_left(k)
            for n, c in ((0, left), (1, right), (3, far)):
                wq_copy(n, wq_tmp, c, c).wait_recv()
            wq_ring.start_own(0)

        @pl.when(s == 6)
        def _():
            wq_ring.forward(0)

        @pl.when(s < 7)
        def _():
            n_load(s + 1).start()

        @pl.when(s == 8)
        def _():
            wq_ring.finish(0)
            for r in range(4):
                wq_mate(r, core).start()

        @pl.when(s >= 2)
        def _():
            b = s - 2
            a_ring.finish(b)
            for c in range(2):
                part[b, c] = jnp.dot(act[b], wd_in[c], preferred_element_type=jnp.float32).astype(part.dtype)

            @pl.when(b < 6)
            def _():
                part_copy(b).start()

        @pl.when(s == 8)
        def _():
            add_residual(0)
            x2_ring.start_own(0)
            for m in range(2):
                for n in range(4):
                    w_mate(n, m, hid).wait_send()
            for r in range(4):
                wq_mate(r, 1 - core).wait_recv()
            for c in wq_loads:
                c.start()

        @pl.when(s == 9)
        def _():
            x2_ring.forward(0)
            add_residual(1)
            x2_ring.start_own(1)

        return carry

    lax.fori_loop(0, 10, step, 0)

    def x2_rows(c, r):
        return x2_out.at[ds(rows_of(c, r), block), :]

    x2_keep = local(xg.at[hid], x2_rows(core, row), 0)
    x2_keep.start()
    x2_mate = remote(xg.at[mate], x2_rows(core, row), one_s.at[1], one_r.at[1], mate_dev)
    x2_mate.start()
    out_ring = Ring(row, dev_y, lambda k, r, h: x2_rows(h, r), or_s, or_r)
    for k in range(N_CHUNK):
        n_ring.drain(k)
    wq_copy(3, wq_tmp, back, via).wait_send()
    for c in wq_loads:
        c.wait()

    def q_rows(r, start, count):
        return ds(rows_of(core, r) + start, count)

    def qy(k, n, r):
        return remote(q_stage.at[k * qc:(k + 1) * qc, ds(r * qb, qb)],
                      qkv_out.at[q_rows(row, k * qc, qc), ds(chip * qb, qb)],
                      qy_s.at[k, n], qy_r.at[k, n], dev_y(r))

    def qy_got(k, n, r):
        return remote(q_stage.at[k * qc:(k + 1) * qc, ds(r * qb, qb)],
                      qkv_out.at[q_rows(r, k * qc, qc), ds(chip * qb, qb)],
                      qy_s.at[k, n], qy_r.at[k, n], dev_y(r))

    q_keep = [local(q_stage.at[k * qc:(k + 1) * qc, ds(row * qb, qb)],
                    qkv_out.at[q_rows(row, k * qc, qc), ds(chip * qb, qb)], 1 + k) for k in range(Q_CHUNK)]
    qh = qc // 2

    q_ring = Ring(chip, dev_x,
                  lambda j, c, h: qkv_out.at[q_rows(lax.rem(row + 4 - j // 2, 4), (j % 2) * qc + h * qh, qh),
                                             ds(c * qb, qb)],
                  qr_s, qr_r)

    def q_mate(j, c):
        rows = ds(rows_of(c, lax.rem(row + 4 - j // 2, 4)) + (j % 2) * qc, qc)
        return remote(qkv_out.at[rows, :], qkv_out.at[rows, :], qd_s.at[j], qd_r.at[j], mate_dev)

    def qkv(k):
        norm(k * qc, qc, 1)
        q_stage[k * qc:(k + 1) * qc, :] = jnp.dot(
            n_own[k * qc:(k + 1) * qc, :], w_in[:, 0:4 * qb], preferred_element_type=jnp.float32).astype(q_stage.dtype)
        for n in (1, 0, 2):
            qy(k, n, lax.rem(row + n + 1, 4)).start()
        q_keep[k].start()
        q_ring.start_own(k, lambda j, h: q_stage.at[k * qc + h * qh:k * qc + (h + 1) * qh, ds(row * qb, qb)])

    def q_next(n, k):
        qy_got(k, n - 1, lax.rem(row + 4 - n, 4)).wait_recv()
        q_ring.start_own(2 * n + k)

    def q_done(n, k):
        q_ring.finish(2 * n + k)
        q_mate(2 * n + k, core).start()

    x2_ring.forward(1)
    x2_ring.finish(0)
    qkv(0)
    x2_ring.finish(1)
    q_ring.forward(0)
    for n in (1, 3):
        q_next(n, 0)
    qkv(1)
    x2_keep.wait()
    remote(xg.at[mate], x2_rows(1 - core, row), one_s.at[1], one_r.at[1], mate_dev).wait_recv()
    out_ring.start_own(0)
    q_next(2, 0)
    for n in (1, 3):
        q_ring.forward(2 * n)
    q_ring.forward(1)
    q_keep[0].wait()
    q_done(0, 0)
    q_next(1, 1)
    q_ring.forward(4)
    q_done(1, 0)
    q_next(3, 1)
    q_ring.forward(3)
    q_done(3, 0)
    q_next(2, 1)
    q_ring.forward(7)
    q_keep[1].wait()
    q_done(0, 1)
    q_done(2, 0)
    out_ring.forward(0)
    q_ring.forward(5)
    q_done(1, 1)
    q_done(3, 1)
    q_done(2, 1)
    out_ring.finish(0)

    for d in range(1, 8):
        gain_copy(d).wait_send()
    for k in range(N_CHUNK):
        xd(k, hid, 1 - core).wait_send()
    wd_mate.wait_send()
    x2_mate.wait_send()
    for m in range(2):
        for n in range(6):
            ref = stage.at[0, m] if n in (0, 1, 4, 5) else w_rows(m, hid)
            remote(ref, ref, wx_s.at[n, m], wx_r.at[n, m], dev_x(right)).wait_send()
    for n in range(3):
        wq_copy(n, wq_tmp, chip, right).wait_send()
    for r in range(4):
        wq_mate(r, core).wait_send()
    for s in range(6):
        part_copy(s).wait_send()
    for k in range(Q_CHUNK):
        for n in range(3):
            qy(k, n, lax.rem(row + n + 1, 4)).wait_send()
        x2_ring.drain(k)
    for j in range(4 * Q_CHUNK):
        q_mate(j, core).wait_send()
        q_ring.drain(j)

    def drain_act(s, carry):
        a_ring.drain(s)
        return carry

    lax.fori_loop(0, 8, drain_act, 0)
    wq_ring.drain(0)
    out_ring.drain(0)
    for j in range(4 * Q_CHUNK):
        q_mate(j, 1 - core).wait_recv()


def solution(mesh):
    hid_ways, ffn_ways = mesh.shape['hid'], mesh.shape['ffn']
    assert hid_ways == 8 and ffn_ways == 4

    def device_step(residual, gain_mlp, gain_attn, w_gate, w_up, w_down, w_qkv):
        tokens, width = residual.shape
        d_model = width * hid_ways
        block, sub = tokens // 8, tokens // 16
        ff, qb = w_gate.shape[1] // 4, w_qkv.shape[1] // 4
        gains = jnp.stack([gain_mlp, gain_attn])
        dtype = residual.dtype
        any_spec = pl.BlockSpec(memory_space=pl.ANY)
        dma = pltpu.SemaphoreType.DMA
        outs = pl.pallas_call(
            functools.partial(kernel, d_model),
            out_shape=(jax.ShapeDtypeStruct((tokens, width), dtype),
                       jax.ShapeDtypeStruct((tokens, w_qkv.shape[1]), dtype),
                       jax.ShapeDtypeStruct((4, block, d_model), dtype),
                       jax.ShapeDtypeStruct((4, 2, 4, width, qb), dtype)),
            in_specs=[any_spec] * 6,
            out_specs=(any_spec,) * 4,
            scratch_shapes=[
                pltpu.VMEM((8, block, width), dtype),
                pltpu.VMEM((block, d_model), dtype),
                pltpu.VMEM((sub, d_model), dtype),
                pltpu.VMEM((d_model, 2 * ff), dtype),
                pltpu.VMEM((2, 2, width // 2, ff), dtype),
                pltpu.VMEM((8, sub, 4 * ff), dtype),
                pltpu.VMEM((2, 4 * ff, width), dtype),
                pltpu.VMEM((8, 2, sub, width), dtype),
                pltpu.VMEM((6, 2, sub, width), dtype),
                pltpu.VMEM((max(block, width), 4 * qb), dtype),
                pltpu.VMEM((8, 2, width), jnp.float32),
                dma((48,)), dma((2,)), dma((2,)), dma((7,)), dma((7,)),
                dma((N_CHUNK,)), dma((N_CHUNK,)), dma((6, 2)), dma((6, 2)), dma((4, 2)), dma((4, 2)),
                dma((4,)), dma((4,)), dma((4,)), dma((4,)), dma((6,)), dma((6,)),
                dma((Q_CHUNK, 3)), dma((Q_CHUNK, 3)), dma((4 * Q_CHUNK,)), dma((4 * Q_CHUNK,)),
                dma((N_CHUNK, 6)), dma((N_CHUNK, 6)), dma((N_CHUNK, 6)), dma((N_CHUNK, 6)),
                dma((8, 6)), dma((8, 6)), dma((1, 6)), dma((1, 6)), dma((Q_CHUNK, 6)), dma((Q_CHUNK, 6)),
                dma((1, 6)), dma((1, 6)), dma((4 * Q_CHUNK, 6)), dma((4 * Q_CHUNK, 6)),
            ],
            compiler_params=pltpu.CompilerParams(
                collective_id=0, has_side_effects=True, vmem_limit_bytes=67043328),
            name='layer',
        )(residual, gains, w_gate, w_up, w_down, w_qkv)
        return outs[0], outs[1]

    return jax.shard_map(
        device_step, mesh=mesh,
        in_specs=(P('data', 'hid'), P('hid'), P('hid'), P('hid', 'ffn'), P('hid', 'ffn'),
                  P('ffn', 'hid'), P('hid', 'ffn')),
        out_specs=(P('data', 'hid'), P('data', 'ffn')),
        check_vma=False)
```

```python
import functools

import jax
import jax.numpy as jnp
from jax import lax
from jax.experimental import pallas as pl
from jax.experimental.pallas import tpu as pltpu
from jax.sharding import PartitionSpec as P

NORM_EPS = 1e-6
MESH = pl.DeviceIdType.MESH
N_CHUNK = 4
Q_CHUNK = 2


class Ring:
    def __init__(self, me, dev, slot, send, recv):
        self.me, self.dev, self.slot, self.send, self.recv = me, dev, slot, send, recv
        self.right, self.left, self.far = (lax.rem(me + d, 4) for d in (1, 3, 2))

    def copy(self, k, n, owner, half, target, src=None):
        dst = self.slot(k, owner, half)
        return pltpu.make_async_remote_copy(
            src_ref=dst if src is None else src, dst_ref=dst,
            send_sem=self.send.at[k, n], recv_sem=self.recv.at[k, n],
            device_id=self.dev(target), device_id_type=MESH)

    def start_own(self, k, src=None, order=(0, 3, 1, 4)):
        for n in order:
            half, target = ((0, self.right), (1, self.right), None, (1, self.left), (0, self.left))[n]
            self.copy(k, n, self.me, half, target, None if src is None else src(k, half)).start()

    def forward(self, k):
        self.copy(k, 0, self.left, 0, self.right).wait_recv()
        self.copy(k, 2, self.left, 0, self.right).start()
        self.copy(k, 3, self.right, 1, self.left).wait_recv()
        self.copy(k, 5, self.right, 1, self.left).start()

    def wait_left(self, k):
        self.copy(k, 1, self.left, 1, self.right).wait_recv()

    def wait_right(self, k):
        self.copy(k, 4, self.right, 0, self.left).wait_recv()

    def wait_far(self, k):
        self.copy(k, 2, self.far, 0, self.right).wait_recv()
        self.copy(k, 5, self.far, 1, self.left).wait_recv()

    def finish(self, k):
        self.wait_left(k)
        self.wait_right(k)
        self.wait_far(k)

    def drain(self, k):
        for n, owner, half, target in ((0, self.me, 0, self.right), (1, self.me, 1, self.right),
                                       (2, self.left, 0, self.right), (3, self.me, 1, self.left),
                                       (4, self.me, 0, self.left), (5, self.right, 1, self.left)):
            self.copy(k, n, owner, half, target).wait_send()


def kernel(d_model, x, gain_a, gain_b, w_gate, w_up, w_down, w_qkv,
           x2_out, qkv_out, n_all, wq_all,
           xg, n_own, n_in, w_in, stage, act, wd_in, part, got, q_stage, gain_buf,
           loc, one_s, one_r, gain_s, gain_r, xd_s, xd_r, wx_s, wx_r, wd_s, wd_r, wq_s, wq_r, wqd_s, wqd_r,
           rs_s, rs_r, qy_s, qy_r, qd_s, qd_r,
           xr_s, xr_r, nr_s, nr_r, ar_s, ar_r, wr_s, wr_r, x2r_s, x2r_r, or_s, or_r, qr_s, qr_r):
    hid, row = lax.axis_index('hid'), lax.axis_index('ffn')
    chip, core = lax.div(hid, 2), lax.rem(hid, 2)
    mate = hid + 1 - 2 * core
    right, left, far = (lax.rem(chip + d, 4) for d in (1, 3, 2))
    tokens, width = x.shape
    half_t, block = tokens // 2, tokens // 8
    sub = block // 2
    ff = w_gate.shape[1] // 4
    qb = w_qkv.shape[1] // 4
    nc, qc = block // N_CHUNK, block // Q_CHUNK

    def dev_x(c):
        return {'hid': 2 * c + core, 'ffn': row}

    def dev_y(r):
        return {'hid': hid, 'ffn': r}

    mate_dev = {'hid': mate, 'ffn': row}

    def remote(src, dst, s, r, dev):
        return pltpu.make_async_remote_copy(src_ref=src, dst_ref=dst, send_sem=s, recv_sem=r,
                                            device_id=dev, device_id_type=MESH)

    def local(src, dst, n):
        return pltpu.make_async_copy(src, dst, loc.at[n])

    def rows_of(c, r):
        return c * half_t + r * block

    def ds(start, size):
        return pl.ds(pl.multiple_of(start, size), size)

    barrier = pltpu.get_barrier_semaphore()
    for d in range(1, 8):
        pl.semaphore_signal(barrier, inc=1, device_id={'hid': lax.rem(hid + d, 8), 'ffn': row}, device_id_type=MESH)
    for d in range(1, 4):
        pl.semaphore_signal(barrier, inc=1, device_id=dev_y(lax.rem(row + d, 4)), device_id_type=MESH)
    pl.semaphore_wait(barrier, 10)

    def x_chunk(k, c):
        return x.at[ds(rows_of(c, row) + k * nc, nc), :]

    def xd(k, h, c):
        return remote(x_chunk(k, c), xg.at[h, k * nc:(k + 1) * nc, :], xd_s.at[k], xd_r.at[k], mate_dev)

    x_own = [local(x_chunk(k, core), xg.at[hid, k * nc:(k + 1) * nc, :], k) for k in range(N_CHUNK)]
    for k in range(N_CHUNK):
        xd(k, hid, 1 - core).start()
        x_own[k].start()

    gains = (gain_a, gain_b)

    def gain_copy(d, m):
        to = lax.rem(hid + d, 8)
        return remote(gains[m], gain_buf.at[m, hid], gain_s.at[d - 1, m], gain_r.at[d - 1, m], {'hid': to, 'ffn': row})

    def gain_got(d, m):
        src = lax.rem(hid + 8 - d, 8)
        return remote(gains[m], gain_buf.at[m, src], gain_s.at[d - 1, m], gain_r.at[d - 1, m], {'hid': src, 'ffn': row})

    gain_own = [local(gains[m], gain_buf.at[m, hid], (4, 15)[m]) for m in range(2)]

    x_ring = Ring(chip, dev_x, lambda k, c, h: xg.at[2 * c + (core if h == 0 else 1 - core), k * nc:(k + 1) * nc, :],
                  xr_s, xr_r)
    for k in range(N_CHUNK):
        x_ring.start_own(k, lambda k, h: x_chunk(k, core), order=(0, 4))
        xd(k, mate, core).wait_recv()
        x_ring.start_own(k, order=(3, 1))
    for m in range(2):
        gain_own[m].start()
        for d in range(1, 8):
            gain_copy(d, m).start()
    for k in range(N_CHUNK):
        x_own[k].wait()

    mats = (w_gate, w_up)

    def cols(m, c):
        return mats[m].at[:, ds(c * ff, ff)]

    def w_rows(m, h):
        return w_in.at[ds(h * width, width), m * ff:(m + 1) * ff]

    w_own = [local(cols(m, chip), w_rows(m, hid), 5 + m) for m in range(2)]
    wd_own = local(w_down, wd_in.at[core], 7)
    for c in (*w_own, wd_own):
        c.start()
    wd_mate = remote(w_down, wd_in.at[core], one_s.at[0], one_r.at[0], mate_dev)
    wd_mate.start()

    def w_mate(n, m, h):
        return remote(w_rows(m, h), w_rows(m, h), wd_s.at[n, m], wd_r.at[n, m], mate_dev)

    for m in range(2):
        remote(cols(m, chip), w_rows(m, hid), wd_s.at[0, m], wd_r.at[0, m], mate_dev).start()

    for k in range(N_CHUNK):
        x_ring.forward(k)

    hw = width // 2

    def far_half(m, side, c):
        return mats[m].at[side * hw:(side + 1) * hw, ds(c * ff, ff)]

    def half_rows(m, h, side):
        return w_in.at[ds(h * width + side * hw, hw), m * ff:(m + 1) * ff]

    for m in range(2):
        remote(far_half(m, 0, far), stage.at[0, m], wx_s.at[0, m], wx_r.at[0, m], dev_x(right)).start()
        remote(far_half(m, 1, far), stage.at[1, m], wx_s.at[1, m], wx_r.at[1, m], dev_x(left)).start()
    for m in range(2):
        remote(cols(m, right), w_rows(m, hid), wx_s.at[2, m], wx_r.at[2, m], dev_x(right)).start()
        remote(cols(m, left), w_rows(m, hid), wx_s.at[3, m], wx_r.at[3, m], dev_x(left)).start()

    wq_in = local(w_qkv.at[:, ds(chip * qb, qb)], q_stage.at[0:width, 0:qb], 8)
    wq_in.start()
    via, back = lax.rem(chip + 1 + 2 * core, 4), lax.rem(chip + 3 - 2 * core, 4)
    wq_tmp = q_stage.at[0:width, qb:2 * qb]

    def wq_copy(n, src, owner, c):
        return remote(src, wq_tmp if n == 2 else wq_all.at[row, core, owner], wq_s.at[n], wq_r.at[n], dev_x(c))

    n_ring = Ring(row, dev_y, lambda k, r, h: n_all.at[r, k * nc + h * (nc // 2):k * nc + (h + 1) * (nc // 2), :],
                  nr_s, nr_r)

    def n_src(k, h):
        return n_own.at[k * nc + h * (nc // 2):k * nc + (h + 1) * (nc // 2), :]

    def norm(start, count, which):
        tile = min(16, count)

        def body(t, carry):
            rows = ds(start + t * tile, tile)
            total = jnp.zeros((tile, 1), jnp.float32)
            for h in range(8):
                piece = xg[h, rows, :].astype(jnp.float32)
                total += jnp.sum(piece * piece, axis=1, keepdims=True)
            scale = lax.rsqrt(total / d_model + NORM_EPS)
            for h in range(8):
                piece = xg[h, rows, :].astype(jnp.float32)
                n_own[rows, h * width:(h + 1) * width] = (
                    piece * scale * gain_buf[which, h]).astype(n_own.dtype)
            return carry

        lax.fori_loop(0, count // tile, body, 0)

    for m in range(2):
        gain_own[m].wait()
        for d in range(1, 8):
            gain_got(d, m).wait_recv()
    n_keep = [local(n_own.at[k * nc:(k + 1) * nc, :], n_all.at[row, k * nc:(k + 1) * nc, :], 9 + k)
              for k in range(N_CHUNK)]
    for k in range(N_CHUNK):
        x_ring.finish(k)
        norm(k * nc, nc, 0)
        n_ring.start_own(k, n_src)
        n_keep[k].start()

    wq_in.wait()
    wq_keep = local(q_stage.at[0:width, 0:qb], wq_all.at[row, core, chip], 8)
    wq_keep.start()

    n_ring.forward(0)
    for m in range(2):
        remote(stage.at[0, m], stage.at[0, m], wx_s.at[0, m], wx_r.at[0, m], dev_x(right)).wait_recv()
        remote(stage.at[0, m], half_rows(m, 2 * left + core, 0), wx_s.at[4, m], wx_r.at[4, m], dev_x(right)).start()
        remote(stage.at[1, m], stage.at[1, m], wx_s.at[1, m], wx_r.at[1, m], dev_x(left)).wait_recv()
        remote(stage.at[1, m], half_rows(m, 2 * right + core, 1), wx_s.at[5, m], wx_r.at[5, m], dev_x(left)).start()
    wq_copy(2, w_qkv.at[:, ds(far * qb, qb)], chip, via).start()
    wq_copy(0, w_qkv.at[:, ds(right * qb, qb)], chip, right).start()
    wq_copy(1, w_qkv.at[:, ds(left * qb, qb)], chip, left).start()
    n_ring.forward(1)
    n_ring.forward(2)
    for m in range(2):
        remote(w_rows(m, hid), w_rows(m, 2 * left + core), wx_s.at[2, m], wx_r.at[2, m], dev_x(right)).wait_recv()
        w_mate(1, m, 2 * left + core).start()
        remote(w_rows(m, hid), w_rows(m, 2 * right + core), wx_s.at[3, m], wx_r.at[3, m], dev_x(left)).wait_recv()
        w_mate(2, m, 2 * right + core).start()
    n_ring.forward(3)
    for m in range(2):
        h = 2 * far + core
        remote(stage.at[0, m], half_rows(m, h, 0), wx_s.at[4, m], wx_r.at[4, m], dev_x(right)).wait_recv()
        remote(stage.at[1, m], half_rows(m, h, 1), wx_s.at[5, m], wx_r.at[5, m], dev_x(left)).wait_recv()
        w_mate(3, m, h).start()
    wq_keep.wait()
    wq_ring = Ring(row, dev_y, lambda k, r, h: wq_all.at[r, core, 2 * h:2 * h + 2], wr_s, wr_r)
    for c in w_own:
        c.wait()
    for m in range(2):
        for n, c in enumerate((chip, left, right, far)):
            w_mate(n, m, 2 * c + 1 - core).wait_recv()
    wd_own.wait()
    remote(w_down, wd_in.at[1 - core], one_s.at[0], one_r.at[0], mate_dev).wait_recv()
    for k in range(N_CHUNK):
        n_keep[k].wait()
        x_ring.drain(k)

    def part_rows(h, start, count):
        return pl.ds(start + h * (count // 2), count // 2)

    a_ring = Ring(chip, dev_x, lambda s, c, h: act.at[s, part_rows(h, 0, sub), ds(c * ff, ff)], ar_s, ar_r)

    def n_load(s):
        r = lax.rem(row + lax.div(s, 2) + 1, 4)
        return local(n_all.at[r, ds(lax.rem(s, 2) * sub, sub), :], n_in, 13)

    def part_copy(s):
        d = lax.div(s, 2) + 1
        to = lax.rem(row + d, 4)
        return remote(part.at[s], got.at[s], rs_s.at[s], rs_r.at[s], dev_y(to))

    for k in range(N_CHUNK):
        n_ring.wait_right(k)
    n_load(0).start()

    x2_ring = Ring(chip, dev_x, lambda k, c, h: xg.at[2 * c + h, k * qc:(k + 1) * qc, :], x2r_s, x2r_r)

    def add_residual(s):
        tile = min(16, sub)
        for q in range(3):
            part_copy(2 * q + s).wait_recv()

        def add(t, carry):
            rows = ds(t * tile, tile)
            out_rows = ds(s * sub + t * tile, tile)
            for c in range(2):
                down = part[6 + s, c, rows, :].astype(jnp.float32)
                for q in range(3):
                    down += got[2 * q + s, c, rows, :].astype(jnp.float32)
                old = xg[2 * chip + c, out_rows, :].astype(jnp.float32)
                xg[2 * chip + c, out_rows, :] = (
                    old + down.astype(jnp.bfloat16).astype(jnp.float32)).astype(xg.dtype)
            return carry

        lax.fori_loop(0, sub // tile, add, 0)

    def wq_mate(r, c):
        return remote(wq_all.at[r, c], wq_all.at[r, c], wqd_s.at[r], wqd_r.at[r], mate_dev)

    wq_loads = [local(wq_all.at[r, c, i], w_in.at[(2 * i + c) * width:(2 * i + c + 1) * width, r * qb:(r + 1) * qb],
                      16 + r * 8 + c * 4 + i) for r in range(4) for c in range(2) for i in range(4)]

    def step(s, carry):
        @pl.when(s < 8)
        def _():
            n_load(s).wait()
            gate = jnp.dot(n_in[...], w_in[:, 0:ff], preferred_element_type=jnp.float32).astype(jnp.bfloat16)
            up = jnp.dot(n_in[...], w_in[:, ff:2 * ff], preferred_element_type=jnp.float32).astype(jnp.bfloat16)
            act[s, :, ds(chip * ff, ff)] = (
                jax.nn.silu(gate.astype(jnp.float32)) * up.astype(jnp.float32)).astype(act.dtype)
            a_ring.start_own(s)

        @pl.when((s >= 1) & (s < 9))
        def _():
            a_ring.forward(s - 1)

        @pl.when(s == 1)
        def _():
            wq_copy(2, w_qkv.at[:, ds(far * qb, qb)], chip, via).wait_recv()
            wq_copy(3, wq_tmp, back, via).start()
            for k in range(N_CHUNK):
                n_ring.wait_far(k)

        @pl.when(s == 3)
        def _():
            for k in range(N_CHUNK):
                n_ring.wait_left(k)
            for n, c in ((0, left), (1, right), (3, far)):
                wq_copy(n, wq_tmp, c, c).wait_recv()
            wq_ring.start_own(0)

        @pl.when(s == 6)
        def _():
            wq_ring.forward(0)

        @pl.when(s < 7)
        def _():
            n_load(s + 1).start()

        @pl.when(s == 8)
        def _():
            wq_ring.finish(0)
            for r in range(4):
                wq_mate(r, core).start()

        @pl.when(s >= 3)
        def _():
            b = s - 3
            a_ring.finish(b)
            for c in range(2):
                part[b, c] = jnp.dot(act[b], wd_in[c], preferred_element_type=jnp.float32).astype(part.dtype)

            @pl.when(b < 6)
            def _():
                part_copy(b).start()

        @pl.when(s == 9)
        def _():
            add_residual(0)
            x2_ring.start_own(0)
            for m in range(2):
                for n in range(4):
                    w_mate(n, m, hid).wait_send()
            for r in range(4):
                wq_mate(r, 1 - core).wait_recv()
            for c in wq_loads:
                c.start()

        @pl.when(s == 10)
        def _():
            x2_ring.forward(0)
            add_residual(1)
            x2_ring.start_own(1)

        return carry

    lax.fori_loop(0, 11, step, 0)

    def x2_rows(c, r):
        return x2_out.at[ds(rows_of(c, r), block), :]

    x2_keep = local(xg.at[hid], x2_rows(core, row), 0)
    x2_keep.start()
    x2_mate = remote(xg.at[mate], x2_rows(core, row), one_s.at[1], one_r.at[1], mate_dev)
    x2_mate.start()
    out_ring = Ring(row, dev_y, lambda k, r, h: x2_rows(h, r), or_s, or_r)
    for k in range(N_CHUNK):
        n_ring.drain(k)
    wq_copy(3, wq_tmp, back, via).wait_send()
    for c in wq_loads:
        c.wait()

    def q_rows(r, start, count):
        return ds(rows_of(core, r) + start, count)

    def qy(k, n, r):
        return remote(q_stage.at[k * qc:(k + 1) * qc, ds(r * qb, qb)],
                      qkv_out.at[q_rows(row, k * qc, qc), ds(chip * qb, qb)],
                      qy_s.at[k, n], qy_r.at[k, n], dev_y(r))

    def qy_got(k, n, r):
        return remote(q_stage.at[k * qc:(k + 1) * qc, ds(r * qb, qb)],
                      qkv_out.at[q_rows(r, k * qc, qc), ds(chip * qb, qb)],
                      qy_s.at[k, n], qy_r.at[k, n], dev_y(r))

    q_keep = [local(q_stage.at[k * qc:(k + 1) * qc, ds(row * qb, qb)],
                    qkv_out.at[q_rows(row, k * qc, qc), ds(chip * qb, qb)], 1 + k) for k in range(Q_CHUNK)]

    q_ring = Ring(chip, dev_x,
                  lambda j, c, h: qkv_out.at[part_rows(h, rows_of(core, lax.rem(row + 4 - j // 2, 4)) + (j % 2) * qc, qc),
                                             ds(c * qb, qb)],
                  qr_s, qr_r)

    def q_mate(j, c):
        rows = ds(rows_of(c, lax.rem(row + 4 - j // 2, 4)) + (j % 2) * qc, qc)
        return remote(qkv_out.at[rows, :], qkv_out.at[rows, :], qd_s.at[j], qd_r.at[j], mate_dev)

    def qkv(k):
        norm(k * qc, qc, 1)
        q_stage[k * qc:(k + 1) * qc, :] = jnp.dot(
            n_own[k * qc:(k + 1) * qc, :], w_in[:, 0:4 * qb], preferred_element_type=jnp.float32).astype(q_stage.dtype)
        for n in (1, 0, 2):
            qy(k, n, lax.rem(row + n + 1, 4)).start()
        q_keep[k].start()
        q_ring.start_own(k, lambda j, h: q_stage.at[part_rows(h, k * qc, qc), ds(row * qb, qb)])

    def q_next(n, k):
        qy_got(k, n - 1, lax.rem(row + 4 - n, 4)).wait_recv()
        q_ring.start_own(2 * n + k)

    def q_done(n, k):
        q_ring.finish(2 * n + k)
        q_mate(2 * n + k, core).start()

    x2_ring.forward(1)
    x2_ring.finish(0)
    qkv(0)
    x2_ring.finish(1)
    q_ring.forward(0)
    for n in (1, 3):
        q_next(n, 0)
    qkv(1)
    x2_keep.wait()
    remote(xg.at[mate], x2_rows(1 - core, row), one_s.at[1], one_r.at[1], mate_dev).wait_recv()
    out_ring.start_own(0)
    q_next(2, 0)
    for n in (1, 3):
        q_ring.forward(2 * n)
    q_ring.forward(1)
    q_keep[0].wait()
    q_done(0, 0)
    q_next(1, 1)
    q_ring.forward(4)
    q_done(1, 0)
    q_next(3, 1)
    q_ring.forward(3)
    q_done(3, 0)
    q_next(2, 1)
    q_ring.forward(7)
    q_keep[1].wait()
    q_done(0, 1)
    q_done(2, 0)
    out_ring.forward(0)
    q_ring.forward(5)
    q_done(1, 1)
    q_done(3, 1)
    q_done(2, 1)
    out_ring.finish(0)

    for d in range(1, 8):
        for m in range(2):
            gain_copy(d, m).wait_send()
    for k in range(N_CHUNK):
        xd(k, hid, 1 - core).wait_send()
    wd_mate.wait_send()
    x2_mate.wait_send()
    for m in range(2):
        for n in range(6):
            ref = stage.at[0, m] if n in (0, 1, 4, 5) else w_rows(m, hid)
            remote(ref, ref, wx_s.at[n, m], wx_r.at[n, m], dev_x(right)).wait_send()
    for n in range(3):
        wq_copy(n, wq_tmp, chip, right).wait_send()
    for r in range(4):
        wq_mate(r, core).wait_send()
    for s in range(6):
        part_copy(s).wait_send()
    for k in range(Q_CHUNK):
        for n in range(3):
            qy(k, n, lax.rem(row + n + 1, 4)).wait_send()
        x2_ring.drain(k)
    for j in range(4 * Q_CHUNK):
        q_mate(j, core).wait_send()
        q_ring.drain(j)

    def drain_act(s, carry):
        a_ring.drain(s)
        return carry

    lax.fori_loop(0, 8, drain_act, 0)
    wq_ring.drain(0)
    out_ring.drain(0)
    for j in range(4 * Q_CHUNK):
        q_mate(j, 1 - core).wait_recv()


def settle_kernel(pieces, a, b, a_out, b_out, a_buf, b_buf, read, write):
    copies = []
    for n, (src, buf, dst) in enumerate(((b, b_buf, b_out), (a, a_buf, a_out))):
        rows = src.shape[0] // pieces
        for p in range(pieces):
            at = pl.ds(p * rows, rows)
            copies.append((pltpu.make_async_copy(src.at[at, :], buf.at[at, :], read.at[n, p]),
                           pltpu.make_async_copy(buf.at[at, :], dst.at[at, :], write.at[n, p])))
    for into, _ in copies:
        into.start()
    for into, out in copies:
        into.wait()
        out.start()
    for _, out in copies:
        out.wait()


def settle(a, b):
    pieces = 8
    spec = pl.BlockSpec(memory_space=pl.ANY)
    dma = pltpu.SemaphoreType.DMA
    return pl.pallas_call(
        functools.partial(settle_kernel, pieces),
        out_shape=(jax.ShapeDtypeStruct(a.shape, a.dtype), jax.ShapeDtypeStruct(b.shape, b.dtype)),
        in_specs=[spec] * 2, out_specs=(spec,) * 2,
        scratch_shapes=[pltpu.VMEM(a.shape, a.dtype), pltpu.VMEM(b.shape, b.dtype), dma((2, pieces)), dma((2, pieces))],
        compiler_params=pltpu.CompilerParams(vmem_limit_bytes=67043328),
        name='settle',
    )(a, b)


def solution(mesh):
    hid_ways, ffn_ways = mesh.shape['hid'], mesh.shape['ffn']
    assert hid_ways == 8 and ffn_ways == 4

    def device_step(residual, gain_mlp, gain_attn, w_gate, w_up, w_down, w_qkv):
        tokens, width = residual.shape
        d_model = width * hid_ways
        block, sub = tokens // 8, tokens // 16
        ff, qb = w_gate.shape[1] // 4, w_qkv.shape[1] // 4
        dtype = residual.dtype
        any_spec = pl.BlockSpec(memory_space=pl.ANY)
        dma = pltpu.SemaphoreType.DMA
        outs = pl.pallas_call(
            functools.partial(kernel, d_model),
            out_shape=(jax.ShapeDtypeStruct((tokens, width), dtype),
                       jax.ShapeDtypeStruct((tokens, w_qkv.shape[1]), dtype),
                       jax.ShapeDtypeStruct((4, block, d_model), dtype),
                       jax.ShapeDtypeStruct((4, 2, 4, width, qb), dtype)),
            in_specs=[any_spec] * 7,
            out_specs=(any_spec,) * 4,
            scratch_shapes=[
                pltpu.VMEM((8, block, width), dtype),
                pltpu.VMEM((block, d_model), dtype),
                pltpu.VMEM((sub, d_model), dtype),
                pltpu.VMEM((d_model, 2 * ff), dtype),
                pltpu.VMEM((2, 2, width // 2, ff), dtype),
                pltpu.VMEM((8, sub, 4 * ff), dtype),
                pltpu.VMEM((2, 4 * ff, width), dtype),
                pltpu.VMEM((8, 2, sub, width), dtype),
                pltpu.VMEM((6, 2, sub, width), dtype),
                pltpu.VMEM((max(block, width), 4 * qb), dtype),
                pltpu.VMEM((2, 8, 1, width), jnp.float32),
                dma((48,)), dma((2,)), dma((2,)), dma((7, 2)), dma((7, 2)),
                dma((N_CHUNK,)), dma((N_CHUNK,)), dma((6, 2)), dma((6, 2)), dma((4, 2)), dma((4, 2)),
                dma((4,)), dma((4,)), dma((4,)), dma((4,)), dma((6,)), dma((6,)),
                dma((Q_CHUNK, 3)), dma((Q_CHUNK, 3)), dma((4 * Q_CHUNK,)), dma((4 * Q_CHUNK,)),
                dma((N_CHUNK, 6)), dma((N_CHUNK, 6)), dma((N_CHUNK, 6)), dma((N_CHUNK, 6)),
                dma((8, 6)), dma((8, 6)), dma((1, 6)), dma((1, 6)), dma((Q_CHUNK, 6)), dma((Q_CHUNK, 6)),
                dma((1, 6)), dma((1, 6)), dma((4 * Q_CHUNK, 6)), dma((4 * Q_CHUNK, 6)),
            ],
            compiler_params=pltpu.CompilerParams(
                collective_id=0, has_side_effects=True, vmem_limit_bytes=67043328),
            name='layer',
        )(residual, gain_mlp[None, :], gain_attn[None, :], w_gate, w_up, w_down, w_qkv)
        return settle(outs[0], outs[1])

    return jax.shard_map(
        device_step, mesh=mesh,
        in_specs=(P('data', 'hid'), P('hid'), P('hid'), P('hid', 'ffn'), P('hid', 'ffn'),
                  P('ffn', 'hid'), P('hid', 'ffn')),
        out_specs=(P('data', 'hid'), P('data', 'ffn')),
        check_vma=False)
```

```python
import functools

import jax
import jax.numpy as jnp
from jax import lax
from jax.experimental import pallas as pl
from jax.experimental.pallas import tpu as pltpu
from jax.sharding import PartitionSpec as P

NORM_EPS = 1e-6
MESH = pl.DeviceIdType.MESH
N_CHUNK = 4
Q_CHUNK = 2


class Ring:
    def __init__(self, me, dev, slot, send, recv):
        self.me, self.dev, self.slot, self.send, self.recv = me, dev, slot, send, recv
        self.right, self.left, self.far = (lax.rem(me + d, 4) for d in (1, 3, 2))

    def copy(self, k, n, owner, half, target, src=None):
        dst = self.slot(k, owner, half)
        return pltpu.make_async_remote_copy(
            src_ref=dst if src is None else src, dst_ref=dst,
            send_sem=self.send.at[k, n], recv_sem=self.recv.at[k, n],
            device_id=self.dev(target), device_id_type=MESH)

    def start_own(self, k, src=None, order=(0, 3, 1, 4)):
        for n in order:
            half, target = ((0, self.right), (1, self.right), None, (1, self.left), (0, self.left))[n]
            self.copy(k, n, self.me, half, target, None if src is None else src(k, half)).start()

    def forward(self, k):
        self.copy(k, 0, self.left, 0, self.right).wait_recv()
        self.copy(k, 2, self.left, 0, self.right).start()
        self.copy(k, 3, self.right, 1, self.left).wait_recv()
        self.copy(k, 5, self.right, 1, self.left).start()

    def wait_left(self, k):
        self.copy(k, 1, self.left, 1, self.right).wait_recv()

    def wait_right(self, k):
        self.copy(k, 4, self.right, 0, self.left).wait_recv()

    def wait_far(self, k):
        self.copy(k, 2, self.far, 0, self.right).wait_recv()
        self.copy(k, 5, self.far, 1, self.left).wait_recv()

    def finish(self, k):
        self.wait_left(k)
        self.wait_right(k)
        self.wait_far(k)

    def drain(self, k):
        for n, owner, half, target in ((0, self.me, 0, self.right), (1, self.me, 1, self.right),
                                       (2, self.left, 0, self.right), (3, self.me, 1, self.left),
                                       (4, self.me, 0, self.left), (5, self.right, 1, self.left)):
            self.copy(k, n, owner, half, target).wait_send()


def kernel(d_model, x, gain_a, gain_b, w_gate, w_up, w_down, w_qkv,
           x2_out, qkv_out, n_all, wq_all,
           xg, n_own, n_in, w_in, stage, act, wd_in, part, got, q_stage, gain_buf,
           loc, one_s, one_r, gain_s, gain_r, xd_s, xd_r, wx_s, wx_r, wd_s, wd_r, wq_s, wq_r, wqd_s, wqd_r,
           rs_s, rs_r, qy_s, qy_r, qd_s, qd_r,
           xr_s, xr_r, nr_s, nr_r, ar_s, ar_r, wr_s, wr_r, x2r_s, x2r_r, or_s, or_r, qr_s, qr_r):
    hid, row = lax.axis_index('hid'), lax.axis_index('ffn')
    chip, core = lax.div(hid, 2), lax.rem(hid, 2)
    mate = hid + 1 - 2 * core
    right, left, far = (lax.rem(chip + d, 4) for d in (1, 3, 2))
    tokens, width = x.shape
    half_t, block = tokens // 2, tokens // 8
    sub = block // 2
    ff = w_gate.shape[1] // 4
    qb = w_qkv.shape[1] // 4
    nc, qc = block // N_CHUNK, block // Q_CHUNK

    def dev_x(c):
        return {'hid': 2 * c + core, 'ffn': row}

    def dev_y(r):
        return {'hid': hid, 'ffn': r}

    mate_dev = {'hid': mate, 'ffn': row}

    def remote(src, dst, s, r, dev):
        return pltpu.make_async_remote_copy(src_ref=src, dst_ref=dst, send_sem=s, recv_sem=r,
                                            device_id=dev, device_id_type=MESH)

    def local(src, dst, n):
        return pltpu.make_async_copy(src, dst, loc.at[n])

    def rows_of(c, r):
        return c * half_t + r * block

    def ds(start, size):
        return pl.ds(pl.multiple_of(start, size), size)

    barrier = pltpu.get_barrier_semaphore()
    for d in range(1, 8):
        pl.semaphore_signal(barrier, inc=1, device_id={'hid': lax.rem(hid + d, 8), 'ffn': row}, device_id_type=MESH)
    for d in range(1, 4):
        pl.semaphore_signal(barrier, inc=1, device_id=dev_y(lax.rem(row + d, 4)), device_id_type=MESH)
    pl.semaphore_wait(barrier, 10)

    def x_chunk(k, c):
        return x.at[ds(rows_of(c, row) + k * nc, nc), :]

    def xd(k, h, c):
        return remote(x_chunk(k, c), xg.at[h, k * nc:(k + 1) * nc, :], xd_s.at[k], xd_r.at[k], mate_dev)

    x_own = [local(x_chunk(k, core), xg.at[hid, k * nc:(k + 1) * nc, :], k) for k in range(N_CHUNK)]
    for k in range(N_CHUNK):
        xd(k, hid, 1 - core).start()
        x_own[k].start()

    gains = (gain_a, gain_b)

    def gain_copy(d, m):
        to = lax.rem(hid + d, 8)
        return remote(gains[m], gain_buf.at[m, hid], gain_s.at[d - 1, m], gain_r.at[d - 1, m], {'hid': to, 'ffn': row})

    def gain_got(d, m):
        src = lax.rem(hid + 8 - d, 8)
        return remote(gains[m], gain_buf.at[m, src], gain_s.at[d - 1, m], gain_r.at[d - 1, m], {'hid': src, 'ffn': row})

    gain_own = [local(gains[m], gain_buf.at[m, hid], (4, 15)[m]) for m in range(2)]

    x_ring = Ring(chip, dev_x, lambda k, c, h: xg.at[2 * c + (core if h == 0 else 1 - core), k * nc:(k + 1) * nc, :],
                  xr_s, xr_r)
    for k in range(N_CHUNK):
        x_ring.start_own(k, lambda k, h: x_chunk(k, core), order=(0, 4))
        xd(k, mate, core).wait_recv()
        x_ring.start_own(k, order=(3, 1))
    for m in range(2):
        gain_own[m].start()
        for d in range(1, 8):
            gain_copy(d, m).start()
    for k in range(N_CHUNK):
        x_own[k].wait()

    mats = (w_gate, w_up)

    def cols(m, c):
        return mats[m].at[:, ds(c * ff, ff)]

    def w_rows(m, h):
        return w_in.at[ds(h * width, width), m * ff:(m + 1) * ff]

    w_own = [local(cols(m, chip), w_rows(m, hid), 5 + m) for m in range(2)]
    wd_own = local(w_down, wd_in.at[core], 7)
    for c in (*w_own, wd_own):
        c.start()
    wd_mate = remote(w_down, wd_in.at[core], one_s.at[0], one_r.at[0], mate_dev)
    wd_mate.start()

    def w_mate(n, m, h):
        return remote(w_rows(m, h), w_rows(m, h), wd_s.at[n, m], wd_r.at[n, m], mate_dev)

    for m in range(2):
        remote(cols(m, chip), w_rows(m, hid), wd_s.at[0, m], wd_r.at[0, m], mate_dev).start()

    for k in range(N_CHUNK):
        x_ring.forward(k)

    hw = width // 2

    def far_half(m, side, c):
        return mats[m].at[side * hw:(side + 1) * hw, ds(c * ff, ff)]

    def half_rows(m, h, side):
        return w_in.at[ds(h * width + side * hw, hw), m * ff:(m + 1) * ff]

    for m in range(2):
        remote(far_half(m, 0, far), stage.at[0, m], wx_s.at[0, m], wx_r.at[0, m], dev_x(right)).start()
        remote(far_half(m, 1, far), stage.at[1, m], wx_s.at[1, m], wx_r.at[1, m], dev_x(left)).start()
    for m in range(2):
        remote(cols(m, right), w_rows(m, hid), wx_s.at[2, m], wx_r.at[2, m], dev_x(right)).start()
        remote(cols(m, left), w_rows(m, hid), wx_s.at[3, m], wx_r.at[3, m], dev_x(left)).start()

    wq_in = local(w_qkv.at[:, ds(chip * qb, qb)], q_stage.at[0:width, 0:qb], 8)
    wq_in.start()
    via, back = lax.rem(chip + 1 + 2 * core, 4), lax.rem(chip + 3 - 2 * core, 4)
    wq_tmp = q_stage.at[0:width, qb:2 * qb]

    def wq_copy(n, src, owner, c):
        return remote(src, wq_tmp if n == 2 else wq_all.at[row, core, owner], wq_s.at[n], wq_r.at[n], dev_x(c))

    n_ring = Ring(row, dev_y, lambda k, r, h: n_all.at[r, k * nc + h * (nc // 2):k * nc + (h + 1) * (nc // 2), :],
                  nr_s, nr_r)

    def n_src(k, h):
        return n_own.at[k * nc + h * (nc // 2):k * nc + (h + 1) * (nc // 2), :]

    def norm(start, count, which):
        tile = min(16, count)

        def body(t, carry):
            rows = ds(start + t * tile, tile)
            total = jnp.zeros((tile, 1), jnp.float32)
            for h in range(8):
                piece = xg[h, rows, :].astype(jnp.float32)
                total += jnp.sum(piece * piece, axis=1, keepdims=True)
            scale = lax.rsqrt(total / d_model + NORM_EPS)
            for h in range(8):
                piece = xg[h, rows, :].astype(jnp.float32)
                n_own[rows, h * width:(h + 1) * width] = (
                    piece * scale * gain_buf[which, h]).astype(n_own.dtype)
            return carry

        lax.fori_loop(0, count // tile, body, 0)

    for m in range(2):
        gain_own[m].wait()
        for d in range(1, 8):
            gain_got(d, m).wait_recv()
    n_keep = [local(n_own.at[k * nc:(k + 1) * nc, :], n_all.at[row, k * nc:(k + 1) * nc, :], 9 + k)
              for k in range(N_CHUNK)]
    for k in range(N_CHUNK):
        x_ring.finish(k)
        norm(k * nc, nc, 0)
        n_ring.start_own(k, n_src)
        n_keep[k].start()

    wq_in.wait()
    wq_keep = local(q_stage.at[0:width, 0:qb], wq_all.at[row, core, chip], 8)
    wq_keep.start()

    n_ring.forward(0)
    for m in range(2):
        remote(stage.at[0, m], stage.at[0, m], wx_s.at[0, m], wx_r.at[0, m], dev_x(right)).wait_recv()
        remote(stage.at[0, m], half_rows(m, 2 * left + core, 0), wx_s.at[4, m], wx_r.at[4, m], dev_x(right)).start()
        remote(stage.at[1, m], stage.at[1, m], wx_s.at[1, m], wx_r.at[1, m], dev_x(left)).wait_recv()
        remote(stage.at[1, m], half_rows(m, 2 * right + core, 1), wx_s.at[5, m], wx_r.at[5, m], dev_x(left)).start()
    wq_copy(2, w_qkv.at[:, ds(far * qb, qb)], chip, via).start()
    wq_copy(0, w_qkv.at[:, ds(right * qb, qb)], chip, right).start()
    wq_copy(1, w_qkv.at[:, ds(left * qb, qb)], chip, left).start()
    n_ring.forward(1)
    n_ring.forward(2)
    for m in range(2):
        remote(w_rows(m, hid), w_rows(m, 2 * left + core), wx_s.at[2, m], wx_r.at[2, m], dev_x(right)).wait_recv()
        w_mate(1, m, 2 * left + core).start()
        remote(w_rows(m, hid), w_rows(m, 2 * right + core), wx_s.at[3, m], wx_r.at[3, m], dev_x(left)).wait_recv()
        w_mate(2, m, 2 * right + core).start()
    n_ring.forward(3)
    for m in range(2):
        h = 2 * far + core
        remote(stage.at[0, m], half_rows(m, h, 0), wx_s.at[4, m], wx_r.at[4, m], dev_x(right)).wait_recv()
        remote(stage.at[1, m], half_rows(m, h, 1), wx_s.at[5, m], wx_r.at[5, m], dev_x(left)).wait_recv()
        w_mate(3, m, h).start()
    wq_keep.wait()
    wq_ring = Ring(row, dev_y, lambda k, r, h: wq_all.at[r, core, 2 * h:2 * h + 2], wr_s, wr_r)
    for c in w_own:
        c.wait()
    for m in range(2):
        for n, c in enumerate((chip, left, right, far)):
            w_mate(n, m, 2 * c + 1 - core).wait_recv()
    wd_own.wait()
    remote(w_down, wd_in.at[1 - core], one_s.at[0], one_r.at[0], mate_dev).wait_recv()
    for k in range(N_CHUNK):
        n_keep[k].wait()
        x_ring.drain(k)

    def part_rows(h, start, count):
        return pl.ds(start + h * (count // 2), count // 2)

    a_ring = Ring(chip, dev_x, lambda s, c, h: act.at[s, part_rows(h, 0, sub), ds(c * ff, ff)], ar_s, ar_r)

    def ahead(s):
        q = lax.div(s, 2)
        return lax.rem(2 * q + 1 + lax.div(q, 2), 4)

    def n_load(s):
        r = lax.rem(row + ahead(s), 4)
        return local(n_all.at[r, ds(lax.rem(s, 2) * sub, sub), :], n_in, 13)

    def part_copy(s):
        to = lax.rem(row + ahead(s), 4)
        return remote(part.at[s], got.at[s], rs_s.at[s], rs_r.at[s], dev_y(to))

    for k in range(N_CHUNK):
        n_ring.wait_right(k)
    n_load(0).start()

    x2_ring = Ring(chip, dev_x, lambda k, c, h: xg.at[2 * c + h, k * qc:(k + 1) * qc, :], x2r_s, x2r_r)

    def add_residual(s):
        tile = min(16, sub)
        for q in range(3):
            part_copy(2 * q + s).wait_recv()

        def add(t, carry):
            rows = ds(t * tile, tile)
            out_rows = ds(s * sub + t * tile, tile)
            for c in range(2):
                down = part[6 + s, c, rows, :].astype(jnp.float32)
                for q in range(3):
                    down += got[2 * q + s, c, rows, :].astype(jnp.float32)
                old = xg[2 * chip + c, out_rows, :].astype(jnp.float32)
                xg[2 * chip + c, out_rows, :] = (
                    old + down.astype(jnp.bfloat16).astype(jnp.float32)).astype(xg.dtype)
            return carry

        lax.fori_loop(0, sub // tile, add, 0)

    def wq_mate(r, c):
        return remote(wq_all.at[r, c], wq_all.at[r, c], wqd_s.at[r], wqd_r.at[r], mate_dev)

    wq_loads = [local(wq_all.at[r, c, i], w_in.at[(2 * i + c) * width:(2 * i + c + 1) * width, r * qb:(r + 1) * qb],
                      16 + r * 8 + c * 4 + i) for r in range(4) for c in range(2) for i in range(4)]

    def step(s, carry):
        @pl.when(s < 8)
        def _():
            n_load(s).wait()
            gate = jnp.dot(n_in[...], w_in[:, 0:ff], preferred_element_type=jnp.float32).astype(jnp.bfloat16)
            up = jnp.dot(n_in[...], w_in[:, ff:2 * ff], preferred_element_type=jnp.float32).astype(jnp.bfloat16)
            act[s, :, ds(chip * ff, ff)] = (
                jax.nn.silu(gate.astype(jnp.float32)) * up.astype(jnp.float32)).astype(act.dtype)
            a_ring.start_own(s)

        @pl.when((s >= 1) & (s < 9))
        def _():
            a_ring.forward(s - 1)

        @pl.when(s == 1)
        def _():
            wq_copy(2, w_qkv.at[:, ds(far * qb, qb)], chip, via).wait_recv()
            wq_copy(3, wq_tmp, back, via).start()
            for k in range(N_CHUNK):
                n_ring.wait_left(k)

        @pl.when(s == 3)
        def _():
            for k in range(N_CHUNK):
                n_ring.wait_far(k)
            for n, c in ((0, left), (1, right), (3, far)):
                wq_copy(n, wq_tmp, c, c).wait_recv()
            wq_ring.start_own(0)

        @pl.when(s == 6)
        def _():
            wq_ring.forward(0)

        @pl.when(s < 7)
        def _():
            n_load(s + 1).start()

        @pl.when(s == 8)
        def _():
            wq_ring.finish(0)
            for r in range(4):
                wq_mate(r, core).start()

        @pl.when(s >= 3)
        def _():
            b = s - 3
            a_ring.finish(b)
            for c in range(2):
                part[b, c] = jnp.dot(act[b], wd_in[c], preferred_element_type=jnp.float32).astype(part.dtype)

            @pl.when(b < 6)
            def _():
                part_copy(b).start()

        @pl.when(s == 9)
        def _():
            add_residual(0)
            x2_ring.start_own(0)
            for m in range(2):
                for n in range(4):
                    w_mate(n, m, hid).wait_send()
            for r in range(4):
                wq_mate(r, 1 - core).wait_recv()
            for c in wq_loads:
                c.start()

        @pl.when(s == 10)
        def _():
            x2_ring.forward(0)
            add_residual(1)
            x2_ring.start_own(1)

        return carry

    lax.fori_loop(0, 11, step, 0)

    def x2_rows(c, r):
        return x2_out.at[ds(rows_of(c, r), block), :]

    x2_keep = local(xg.at[hid], x2_rows(core, row), 0)
    x2_keep.start()
    x2_mate = remote(xg.at[mate], x2_rows(core, row), one_s.at[1], one_r.at[1], mate_dev)
    x2_mate.start()
    out_ring = Ring(row, dev_y, lambda k, r, h: x2_rows(h, r), or_s, or_r)
    for k in range(N_CHUNK):
        n_ring.drain(k)
    wq_copy(3, wq_tmp, back, via).wait_send()
    for c in wq_loads:
        c.wait()

    def q_rows(r, start, count):
        return ds(rows_of(core, r) + start, count)

    def qy(k, n, r):
        return remote(q_stage.at[k * qc:(k + 1) * qc, ds(r * qb, qb)],
                      qkv_out.at[q_rows(row, k * qc, qc), ds(chip * qb, qb)],
                      qy_s.at[k, n], qy_r.at[k, n], dev_y(r))

    def qy_got(k, n, r):
        return remote(q_stage.at[k * qc:(k + 1) * qc, ds(r * qb, qb)],
                      qkv_out.at[q_rows(r, k * qc, qc), ds(chip * qb, qb)],
                      qy_s.at[k, n], qy_r.at[k, n], dev_y(r))

    q_keep = [local(q_stage.at[k * qc:(k + 1) * qc, ds(row * qb, qb)],
                    qkv_out.at[q_rows(row, k * qc, qc), ds(chip * qb, qb)], 1 + k) for k in range(Q_CHUNK)]

    q_ring = Ring(chip, dev_x,
                  lambda j, c, h: qkv_out.at[part_rows(h, rows_of(core, lax.rem(row + 4 - j // 2, 4)) + (j % 2) * qc, qc),
                                             ds(c * qb, qb)],
                  qr_s, qr_r)

    def q_mate(j, c):
        rows = ds(rows_of(c, lax.rem(row + 4 - j // 2, 4)) + (j % 2) * qc, qc)
        return remote(qkv_out.at[rows, :], qkv_out.at[rows, :], qd_s.at[j], qd_r.at[j], mate_dev)

    def qkv(k):
        norm(k * qc, qc, 1)
        q_stage[k * qc:(k + 1) * qc, :] = jnp.dot(
            n_own[k * qc:(k + 1) * qc, :], w_in[:, 0:4 * qb], preferred_element_type=jnp.float32).astype(q_stage.dtype)
        for n in (1, 0, 2):
            qy(k, n, lax.rem(row + n + 1, 4)).start()
        q_keep[k].start()
        q_ring.start_own(k, lambda j, h: q_stage.at[part_rows(h, k * qc, qc), ds(row * qb, qb)])

    def q_next(n, k):
        qy_got(k, n - 1, lax.rem(row + 4 - n, 4)).wait_recv()
        q_ring.start_own(2 * n + k)

    def q_done(n, k):
        q_ring.finish(2 * n + k)
        q_mate(2 * n + k, core).start()

    x2_ring.forward(1)
    x2_ring.finish(0)
    qkv(0)
    x2_ring.finish(1)
    q_ring.forward(0)
    for n in (1, 3):
        q_next(n, 0)
    qkv(1)
    x2_keep.wait()
    remote(xg.at[mate], x2_rows(1 - core, row), one_s.at[1], one_r.at[1], mate_dev).wait_recv()
    out_ring.start_own(0)
    q_next(2, 0)
    for n in (1, 3):
        q_ring.forward(2 * n)
    q_ring.forward(1)
    q_keep[0].wait()
    q_done(0, 0)
    q_next(1, 1)
    q_ring.forward(4)
    q_done(1, 0)
    q_next(3, 1)
    q_ring.forward(3)
    q_done(3, 0)
    q_next(2, 1)
    q_ring.forward(7)
    q_keep[1].wait()
    q_done(0, 1)
    q_done(2, 0)
    out_ring.forward(0)
    q_ring.forward(5)
    q_done(1, 1)
    q_done(3, 1)
    q_done(2, 1)
    out_ring.finish(0)

    for d in range(1, 8):
        for m in range(2):
            gain_copy(d, m).wait_send()
    for k in range(N_CHUNK):
        xd(k, hid, 1 - core).wait_send()
    wd_mate.wait_send()
    x2_mate.wait_send()
    for m in range(2):
        for n in range(6):
            ref = stage.at[0, m] if n in (0, 1, 4, 5) else w_rows(m, hid)
            remote(ref, ref, wx_s.at[n, m], wx_r.at[n, m], dev_x(right)).wait_send()
    for n in range(3):
        wq_copy(n, wq_tmp, chip, right).wait_send()
    for r in range(4):
        wq_mate(r, core).wait_send()
    for s in range(6):
        part_copy(s).wait_send()
    for k in range(Q_CHUNK):
        for n in range(3):
            qy(k, n, lax.rem(row + n + 1, 4)).wait_send()
        x2_ring.drain(k)
    for j in range(4 * Q_CHUNK):
        q_mate(j, core).wait_send()
        q_ring.drain(j)

    def drain_act(s, carry):
        a_ring.drain(s)
        return carry

    lax.fori_loop(0, 8, drain_act, 0)
    wq_ring.drain(0)
    out_ring.drain(0)
    for j in range(4 * Q_CHUNK):
        q_mate(j, 1 - core).wait_recv()


def settle_kernel(pieces, a, b, a_out, b_out, a_buf, b_buf, read, write):
    copies = []
    for n, (src, buf, dst) in enumerate(((b, b_buf, b_out), (a, a_buf, a_out))):
        rows = src.shape[0] // pieces
        for p in range(pieces):
            at = pl.ds(p * rows, rows)
            copies.append((pltpu.make_async_copy(src.at[at, :], buf.at[at, :], read.at[n, p]),
                           pltpu.make_async_copy(buf.at[at, :], dst.at[at, :], write.at[n, p])))
    for into, _ in copies:
        into.start()
    for into, out in copies:
        into.wait()
        out.start()
    for _, out in copies:
        out.wait()


def settle(a, b):
    pieces = 8
    spec = pl.BlockSpec(memory_space=pl.ANY)
    dma = pltpu.SemaphoreType.DMA
    return pl.pallas_call(
        functools.partial(settle_kernel, pieces),
        out_shape=(jax.ShapeDtypeStruct(a.shape, a.dtype), jax.ShapeDtypeStruct(b.shape, b.dtype)),
        in_specs=[spec] * 2, out_specs=(spec,) * 2,
        scratch_shapes=[pltpu.VMEM(a.shape, a.dtype), pltpu.VMEM(b.shape, b.dtype), dma((2, pieces)), dma((2, pieces))],
        compiler_params=pltpu.CompilerParams(vmem_limit_bytes=67043328),
        name='settle',
    )(a, b)


def solution(mesh):
    hid_ways, ffn_ways = mesh.shape['hid'], mesh.shape['ffn']
    assert hid_ways == 8 and ffn_ways == 4

    def device_step(residual, gain_mlp, gain_attn, w_gate, w_up, w_down, w_qkv):
        tokens, width = residual.shape
        d_model = width * hid_ways
        block, sub = tokens // 8, tokens // 16
        ff, qb = w_gate.shape[1] // 4, w_qkv.shape[1] // 4
        dtype = residual.dtype
        any_spec = pl.BlockSpec(memory_space=pl.ANY)
        dma = pltpu.SemaphoreType.DMA
        outs = pl.pallas_call(
            functools.partial(kernel, d_model),
            out_shape=(jax.ShapeDtypeStruct((tokens, width), dtype),
                       jax.ShapeDtypeStruct((tokens, w_qkv.shape[1]), dtype),
                       jax.ShapeDtypeStruct((4, block, d_model), dtype),
                       jax.ShapeDtypeStruct((4, 2, 4, width, qb), dtype)),
            in_specs=[any_spec] * 7,
            out_specs=(any_spec,) * 4,
            scratch_shapes=[
                pltpu.VMEM((8, block, width), dtype),
                pltpu.VMEM((block, d_model), dtype),
                pltpu.VMEM((sub, d_model), dtype),
                pltpu.VMEM((d_model, 2 * ff), dtype),
                pltpu.VMEM((2, 2, width // 2, ff), dtype),
                pltpu.VMEM((8, sub, 4 * ff), dtype),
                pltpu.VMEM((2, 4 * ff, width), dtype),
                pltpu.VMEM((8, 2, sub, width), dtype),
                pltpu.VMEM((6, 2, sub, width), dtype),
                pltpu.VMEM((max(block, width), 4 * qb), dtype),
                pltpu.VMEM((2, 8, 1, width), jnp.float32),
                dma((48,)), dma((2,)), dma((2,)), dma((7, 2)), dma((7, 2)),
                dma((N_CHUNK,)), dma((N_CHUNK,)), dma((6, 2)), dma((6, 2)), dma((4, 2)), dma((4, 2)),
                dma((4,)), dma((4,)), dma((4,)), dma((4,)), dma((6,)), dma((6,)),
                dma((Q_CHUNK, 3)), dma((Q_CHUNK, 3)), dma((4 * Q_CHUNK,)), dma((4 * Q_CHUNK,)),
                dma((N_CHUNK, 6)), dma((N_CHUNK, 6)), dma((N_CHUNK, 6)), dma((N_CHUNK, 6)),
                dma((8, 6)), dma((8, 6)), dma((1, 6)), dma((1, 6)), dma((Q_CHUNK, 6)), dma((Q_CHUNK, 6)),
                dma((1, 6)), dma((1, 6)), dma((4 * Q_CHUNK, 6)), dma((4 * Q_CHUNK, 6)),
            ],
            compiler_params=pltpu.CompilerParams(
                collective_id=0, has_side_effects=True, vmem_limit_bytes=67043328),
            name='layer',
        )(residual, gain_mlp[None, :], gain_attn[None, :], w_gate, w_up, w_down, w_qkv)
        return settle(outs[0], outs[1])

    return jax.shard_map(
        device_step, mesh=mesh,
        in_specs=(P('data', 'hid'), P('hid'), P('hid'), P('hid', 'ffn'), P('hid', 'ffn'),
                  P('ffn', 'hid'), P('hid', 'ffn')),
        out_specs=(P('data', 'hid'), P('data', 'ffn')),
        check_vma=False)
```
